32 devices in a mesh: sweep: 2 (over x), expert: 4 (over y, core), fsdp: 4 (over z).
Axes of the slice: x: 2, y: 2, z: 4, core: 2. Of those that a mesh axis runs over, the one named last changes fastest.
Arguments:
- tokens: bfloat16 [4096, 2048], P(('sweep', 'expert', 'fsdp')), parts along dimension 0, may hold values from -6 to 6
- context: bfloat16 [4096, 2048], P(('sweep', 'expert', 'fsdp')), parts along dimension 0, may hold values from -6 to 6
- out_proj: bfloat16 [4096, 2048], P(('sweep', 'expert', 'fsdp')), parts along dimension 0, may hold values from -0.125 to 0.125
- norm_gain: float32 [4096], P('sweep'), parts along dimension 0, may hold values from 0.1 to 1.9
- router: bfloat16 [4096, 8], P('sweep'), parts along dimension 0, may hold values from -0.125 to 0.125
- expert_ids: int32 [4096, 2], P(('sweep', 'expert', 'fsdp')), parts along dimension 0, may hold values from 0 to 7, all different within a row; in each aligned block of 128 rows (0 to 127, 128 to 255, ...) at most 40 rows name the same one
- w_gate_up: bfloat16 [32, 2, 704, 2048], P(('sweep', 'expert', 'fsdp')), parts along dimension 0, may hold values from -0.125 to 0.125
- w_down: bfloat16 [32, 704, 2048], P(('sweep', 'expert', 'fsdp')), parts along dimension 0, may hold values from -0.15625 to 0.15625
Outputs:
- layer_out: bfloat16 [4096, 2048], P(('sweep', 'expert', 'fsdp')), parts along dimension 0
The draws below stay inside these ranges and needn't reach their ends.
There are 2 independent parts, one for each index of `sweep`. The reference program is written for one: setup_inputs(seed, part) draws one part's arguments, and reference() takes and returns one part's arrays. A program takes and returns all parts, laid end to end along the dimension named above; each array names one. Nothing has to cross between parts.
Inputs may be any that keep to these rules, and one draw needn't show every extreme that they name: `expert_ids`: each row names two different experts. Among the rows of one device no expert is named more than 40 times, a bound that some block reaches.
All inputs are finite; a program needn't handle non-finite values.
Results may differ from the reference program's by a relative error of at most 0.012.
Values may be sent and summed in bfloat16 or wider, within the bound.
A program may use at most 64 MiB of HBM per device.

```python
import math
import jax
import jax.numpy as jnp
import numpy as np
from jax import lax

D = 2048
FF = 1408
EXPERTS = 8
TOK_DEV = 128
CAP = 40
TOKENS = 2048
N_EXPERT = 4
N_FSDP = 4


def block_scale(own_key, dims, cuts, least, high):
    def one(dim, blocks):
        steps = jax.random.uniform(jax.random.fold_in(jax.random.fold_in(own_key, 6), dim), (blocks,), jnp.float32, least / len(cuts), high / len(cuts))
        return jnp.repeat(jnp.exp(steps), dims[dim] // blocks).reshape((-1,) + (1,) * (len(dims) - dim - 1))

    factor_of = one(*cuts[0])
    for cut in cuts[1:]:
        factor_of = factor_of * one(*cut)
    return factor_of


def assign_block(own_key, own, number, rows, number_of, top, most, skew):
    order = jax.random.permutation(own_key, number_of)
    packed, ordinary = portions_of(number_of, rows * top, most, skew, True), portions_of(number_of, rows * top, most, skew, False)
    places = jnp.arange(number_of)

    def named(lengths, turn):
        used = int((lengths > 0).sum())
        fixed = max(1, used // 4)
        moved = fixed + (places - fixed + turn * (used - fixed)) % max(1, number_of - fixed)
        return jnp.zeros((number_of,), jnp.int32).at[order[jnp.where(places < fixed, places, moved)]].set(jnp.asarray(lengths, jnp.int32))

    lengths = jnp.where(number % 4 == 0, named(packed, number // 4), named(ordinary, number - number // 4 - 1))
    mixed = jax.random.permutation(jax.random.fold_in(own, 3), number_of)
    giver, receiver = mixed[0:number_of // 2 * 2:2], mixed[1:number_of // 2 * 2:2]
    margin = jnp.minimum(lengths[giver] - 1, most - lengths[receiver]) // 2
    margin = jnp.where((giver == order[0]) | (receiver == order[0]) | (lengths[receiver] == 0), 0, jnp.maximum(margin, 0))
    moved = jax.random.randint(jax.random.fold_in(own, 4), (number_of // 2,), 0, 1 << 20) % (margin + 1)
    lengths = lengths.at[giver].add(-moved).at[receiver].add(moved)
    items = jnp.searchsorted(jnp.cumsum(lengths), jnp.arange(rows * top), side="right").astype(jnp.int32)
    listing = items.reshape(top, rows).T
    listing = listing[jax.random.permutation(jax.random.fold_in(own, 1), rows)]
    turn = jax.random.randint(jax.random.fold_in(own, 2), (rows, 1), 0, top)
    return jnp.take_along_axis(listing, (jnp.arange(top)[None, :] + turn) % top, axis=1)


def portions_of(count, total, limit, skew, full):
    weights = [(1 << 20) // math.isqrt(standing ** skew) + 1 for standing in range(1, count + 1)]
    largest = limit if full else min(limit, max(-(-total // count), total * weights[0] // sum(weights)))
    least = 1 if total - largest >= count - 1 else 0
    counts, spare = [largest] + [least] * (count - 1), total - largest - least * (count - 1)
    while spare > 0:
        movable = [i for i in range(1, count) if counts[i] < largest] or [i for i in range(1, count) if counts[i] < limit]
        mass, left = sum([weights[i] for i in movable]), spare
        for i in movable:
            more = min(limit - counts[i], max(1, left * weights[i] // mass), spare)
            counts[i] = counts[i] + more
            spare = spare - more
    return np.array(counts)


def scatter_about(rng, shape, scale, most, split=(), held_as=jnp.bfloat16):
    entries = scale * jax.random.normal(rng, shape, jnp.float32)
    if split:
        entries = entries * block_scale(rng, shape, split, -0.22, 0.18)
    return jnp.clip(entries, -most, most).astype(held_as)


def setup_inputs(seed: int = 0, part: int = 0) -> dict:
    keys = jax.random.split(jax.random.key(seed), 9)
    part_keys = jax.random.split(jax.random.fold_in(keys[8], part), 9)
    tokens = scatter_about(part_keys[0], (TOKENS, D), 1.0, 6.0, ((0, 16),))
    context = scatter_about(part_keys[1], (TOKENS, D), 1.0, 6.0, ((0, 16),))
    out_proj = scatter_about(part_keys[2], (D, D), D ** -0.5, 0.125, ((0, 16),))
    norm_gain = jnp.clip(1.0 + 0.18 * jax.random.normal(part_keys[3], (D,), jnp.float32), 0.1, 1.9)
    router = scatter_about(part_keys[4], (D, EXPERTS), D ** -0.5, 0.125)
    expert_ids_keys = jax.random.split(jax.random.fold_in(part_keys[5], 1), TOKENS // TOK_DEV)
    expert_ids_turns = jax.random.permutation(jax.random.fold_in(part_keys[5], 3), TOKENS // TOK_DEV)
    expert_ids = jax.vmap(lambda own, number: assign_block(jax.random.fold_in(part_keys[5], 2), own, number, TOK_DEV, EXPERTS, 2, CAP, 2))(expert_ids_keys, expert_ids_turns).reshape((TOKENS, 2))
    w_gate_up = scatter_about(part_keys[6], (2 * EXPERTS, 2, FF // 2, D), D ** -0.5, 0.125, ((0, 16),))
    w_down = scatter_about(part_keys[7], (2 * EXPERTS, FF // 2, D), FF ** -0.5, 0.15625, ((0, 16),))
    return dict(tokens=tokens, context=context, out_proj=out_proj, norm_gain=norm_gain, router=router, expert_ids=expert_ids, w_gate_up=w_gate_up, w_down=w_down)


def reference(tokens, context, out_proj, norm_gain, router, expert_ids, w_gate_up, w_down):
    attended = jnp.dot(context, out_proj, preferred_element_type=jnp.float32)
    residual_in = (tokens.astype(jnp.float32) + attended).astype(jnp.bfloat16)
    widened = residual_in.astype(jnp.float32)
    inv_rms = lax.rsqrt(lax.optimization_barrier(jnp.mean(widened * widened, axis=1, keepdims=True)) + 1e-05)
    normed = (widened * inv_rms * norm_gain).astype(jnp.bfloat16)
    logits = jnp.dot(normed, router, preferred_element_type=jnp.float32)
    picked = jnp.take_along_axis(logits, expert_ids, axis=1)
    scores = jax.nn.sigmoid(picked)
    gate_vals = scores / lax.optimization_barrier(jnp.sum(scores, axis=1, keepdims=True))
    experts = EXPERTS
    blocks = N_EXPERT * N_FSDP
    ids_block = expert_ids.reshape(blocks, 2 * TOK_DEV)
    onehot = (ids_block[:, :, None] == jnp.arange(experts, dtype=jnp.int32)[None, None, :]).astype(jnp.int32)
    before = jnp.cumsum(onehot, axis=1) - onehot
    places = lax.optimization_barrier(jnp.sum(before * onehot, axis=2))
    block_of = jnp.arange(blocks, dtype=jnp.int32)[:, None]
    slot_index = ((ids_block * blocks + block_of) * CAP + places).reshape(-1).astype(jnp.int32)
    assign = jnp.arange(2 * TOKENS, dtype=jnp.int32)
    table_tok = jnp.full((experts * blocks * CAP,), TOKENS, jnp.int32).at[slot_index].set(assign // 2)
    table_gate = jnp.zeros((experts * blocks * CAP,), jnp.float32).at[slot_index].set(gate_vals.reshape(-1))
    padded = jnp.concatenate([normed, jnp.zeros((1, D), jnp.bfloat16)], axis=0)
    half_units = FF // 2

    def one_expert(running, inputs):
        slot_tokens, slot_gates, gate_up_w, down_w = inputs
        taken = padded[slot_tokens]
        total = jnp.zeros((taken.shape[0], D), jnp.float32)
        for half in range(2):
            gate_val = jnp.dot(taken, gate_up_w[half, 0].T, preferred_element_type=jnp.float32)
            up_val = jnp.dot(taken, gate_up_w[half, 1].T, preferred_element_type=jnp.float32)
            hidden = (jax.nn.silu(gate_val) * up_val).astype(jnp.bfloat16)
            piece = jnp.dot(hidden, down_w[half], preferred_element_type=jnp.float32).astype(jnp.bfloat16)
            piece = lax.optimization_barrier(piece)
            total = total + piece.astype(jnp.float32)
        combined = lax.optimization_barrier(total.astype(jnp.bfloat16)).astype(jnp.float32)
        running = running.at[slot_tokens].add(slot_gates[:, None] * combined)
        return (running, None)
    start_acc = jnp.zeros((TOKENS + 1, D), jnp.float32)
    running, unused = lax.scan(one_expert, start_acc, (table_tok.reshape(experts, -1), table_gate.reshape(experts, -1), w_gate_up.reshape(experts, 2, 2, half_units, D), w_down.reshape(experts, 2, half_units, D)))
    return (widened + running[:TOKENS]).astype(jnp.bfloat16)
```

```python
import functools

import jax
import jax.numpy as jnp
from jax import lax
from jax.experimental import pallas as pl
from jax.experimental.pallas import tpu as pltpu
from jax.sharding import PartitionSpec as P

eps_norm = 1e-05
MESH = pl.DeviceIdType.MESH
VMEM_GRANT = 62 * 1024 * 1024
NT = (((1,), (1,)), ((), ()))
TN = (((0,), (0,)), ((), ()))


def both(a, b):
    return jnp.logical_and(a, b)


def inside(i, n):
    return both(i >= 0, i < n)


def block_kernel(
    columns, members, slots, col,
    tok, ctx, wout, gain, router, ids, gu_hbm, dn_hbm,
    out,
    gath, ctxs, acc, pout, pin, gu, dn, resid,
    idsb, hot, mask, gates, tokb, outb, inb, hid, part, back, total, rs_out, rs_in,
    load_sem, w_send, w_recv, id_send, id_recv, c_send, c_recv, p_send, p_recv,
    t_send, t_recv, b_send, b_recv, r_send, r_recv, s_send, s_recv,
):
    lines = columns // 2
    pairs = members // 2
    experts = columns * pairs
    rows, width = tok.shape
    k_rows = wout.shape[0]
    depth = 2 * members * k_rows
    chunks = width // col
    my_e = lax.axis_index("expert")
    my_f = lax.axis_index("fsdp")
    my_y, my_c = lax.div(my_e, 2), lax.rem(my_e, 2)
    my_p = lax.div(my_f, 2)
    other = my_y * 2 + 1 - my_c

    def dev(e, f):
        return {"expert": e, "fsdp": f}

    def span(j):
        return pl.ds(pl.multiple_of(j * col, col), col)

    def copy(src, dst, send, recv, target):
        return pltpu.make_async_remote_copy(
            src_ref=src, dst_ref=dst, send_sem=send, recv_sem=recv,
            device_id=target, device_id_type=MESH)

    def loop(lo, hi, body):
        def one(i, _):
            body(i)
            return 0

        lax.fori_loop(lo, hi, one, 0)

    load_gu = pltpu.make_async_copy(gu_hbm.at[0], gu, load_sem.at[0])
    load_dn = pltpu.make_async_copy(dn_hbm.at[0], dn, load_sem.at[1])

    barrier = pltpu.get_barrier_semaphore()

    def greet(e, f):
        pl.semaphore_signal(barrier, inc=1, device_id=dev(e, f), device_id_type=MESH)

    for sign in (1, -1):
        @pl.when(inside(my_f + sign, members))
        def _():
            greet(my_e, my_f + sign)

    loop(1, columns, lambda i: greet(lax.rem(my_e + i, columns), my_f))
    beside = jnp.where(my_f > 0, 1, 0) + jnp.where(my_f < members - 1, 1, 0)
    pl.semaphore_wait(barrier, columns - 1 + beside)

    def place(c, f):
        return pl.ds(pl.multiple_of((c * members + f) * k_rows, k_rows), k_rows)

    def w_copy(f, j, way, target, own=False):
        at = gath.at[place(my_c, f), span(j)]
        return copy(wout.at[:, span(j)] if own else at, at,
                    w_send.at[f, j, way], w_recv.at[my_c, f, j], target)

    def w_arrived(c, f, j):
        at = gath.at[place(c, f), span(j)]
        copy(at, at, w_send.at[f, j, 0], w_recv.at[c, f, j], dev(other, my_f)).wait_recv()

    def id_copy(f, way, target, own=False):
        return copy(ids if own else idsb.at[f], idsb.at[f], id_send.at[f, way], id_recv.at[f], target)

    def ctx_copy(r):
        line = lax.rem(my_y + r, lines)
        at = pl.ds(pl.multiple_of(line * depth, depth), depth)
        return copy(ctx.at[:, at], ctxs.at[lines - r], c_send.at[r], c_recv.at[lines - r],
                    dev(line * 2 + my_c, my_f))

    def w_start(j, finish):
        for way, sign in ((0, 1), (1, -1)):
            to = my_f + sign

            @pl.when(inside(to, members))
            def _():
                mine = w_copy(my_f, j, way, dev(my_e, to), True)
                mine.wait_send() if finish else mine.start()
        mine = w_copy(my_f, j, 2, dev(other, my_f), True)
        mine.wait_send() if finish else mine.start()

    def id_start(finish):
        for way, sign in ((0, 1), (1, -1)):
            to = my_f + sign

            @pl.when(inside(to, members))
            def _():
                mine = id_copy(my_f, way, dev(my_e, to), True)
                mine.wait_send() if finish else mine.start()

    def w_step(s, j, finish=False):
        for way, sign in ((0, 1), (1, -1)):
            fb, to = my_f - sign * s, my_f + sign

            @pl.when(inside(fb, members))
            def _():
                if not finish:
                    w_arrived(my_c, fb, j)

                    @pl.when(j == 0)
                    def _():
                        id_copy(fb, way, dev(my_e, my_f)).wait_recv()

                @pl.when(inside(to, members))
                def _():
                    onward = w_copy(fb, j, way, dev(my_e, to))
                    onward.wait_send() if finish else onward.start()

                    @pl.when(j == 0)
                    def _():
                        named = id_copy(fb, way, dev(my_e, to))
                        named.wait_send() if finish else named.start()

                across = w_copy(fb, j, 2, dev(other, my_f))
                across.wait_send() if finish else across.start()

    loop(0, chunks, lambda j: w_start(j, False))
    id_start(False)
    for r in range(1, lines):
        ctx_copy(r).start()
    load_gu.start()
    load_dn.start()
    loop(0, chunks, lambda j: gath.__setitem__((place(my_c, my_f), span(j)), wout[:, span(j)]))
    idsb[my_f] = ids[...]
    ctxs[0] = ctx[:, pl.ds(pl.multiple_of(my_y * depth, depth), depth)]
    loop(0, (members - 2) * chunks, lambda i: w_step(1 + lax.div(i, chunks), lax.rem(i, chunks)))
    for r in range(1, lines):
        ctx_copy(r).wait_recv()

    def group_of(k):
        m = jnp.minimum(my_f, members - 1 - my_f)
        half = lax.div(k + 1, 2)
        near = jnp.where(lax.rem(k, 2) == 1, my_f - half, my_f + half)
        far = jnp.where(my_f > m, my_f - (k - m), my_f + (k - m))
        return jnp.where(k <= 2 * m, near, far)

    def make_masks(f):
        diagonal = jnp.where(
            lax.broadcasted_iota(jnp.int32, (rows, rows), 0) == lax.broadcasted_iota(jnp.int32, (rows, rows), 1),
            1.0, 0.0)
        names = idsb[f].astype(jnp.float32)
        id0 = jnp.sum(diagonal * names[0:1], axis=1, keepdims=True).astype(jnp.int32)
        id1 = jnp.sum(diagonal * names[1:2], axis=1, keepdims=True).astype(jnp.int32)
        every = lax.broadcasted_iota(jnp.int32, (rows, experts), 1)
        hot[f, 0] = jnp.where(every == id0, 1.0, 0.0)
        hot[f, 1] = jnp.where(every == id1, 1.0, 0.0)
        place_no = lax.broadcasted_iota(jnp.int32, (rows, columns), 1)
        here = place_no * pairs + my_p
        hot0 = jnp.where(here == id0, 1.0, 0.0)
        hot1 = jnp.where(here == id1, 1.0, 0.0)
        earlier = jnp.where(
            lax.broadcasted_iota(jnp.int32, (rows, rows), 1) < lax.broadcasted_iota(jnp.int32, (rows, rows), 0),
            1.0, 0.0).astype(jnp.bfloat16)
        before = jnp.dot(earlier, (hot0 + hot1).astype(jnp.bfloat16), preferred_element_type=jnp.float32)
        spot = before + (place_no * slots + 1).astype(jnp.float32)
        slot0 = jnp.sum(spot * hot0, axis=1, keepdims=True).astype(jnp.int32) - 1
        slot1 = jnp.sum(spot * hot1, axis=1, keepdims=True).astype(jnp.int32) - 1
        slot_no = lax.broadcasted_iota(jnp.int32, (rows, columns * slots), 1)
        mask[f, 0] = jnp.where(slot_no == slot0, 1.0, 0.0).astype(jnp.bfloat16)
        mask[f, 1] = jnp.where(slot_no == slot1, 1.0, 0.0).astype(jnp.bfloat16)

    def part_copy(r, j):
        line = lax.rem(my_y + r, lines)
        return copy(pout.at[r - 1, :, span(j)], pin.at[lines - r - 1, :, span(j)],
                    p_send.at[r - 1, j], p_recv.at[lines - r - 1, j], dev(line * 2 + my_c, my_f))

    def project(j):
        loop(lax.div(j * members, chunks), lax.div((j + 1) * members, chunks),
             lambda k: make_masks(group_of(k)))
        w_step(members - 1, j)
        loop(0, members, lambda f: w_arrived(1 - my_c, f, j))
        mixed = jnp.dot(ctxs[...].reshape(lines * rows, depth), gath[:, span(j)],
                        preferred_element_type=jnp.float32)
        for r in range(1, lines):
            pout[r - 1, :, span(j)] = mixed[r * rows:(r + 1) * rows].astype(jnp.bfloat16)
            part_copy(r, j).start()
        acc[:, span(j)] = mixed[:rows] + tok[:, span(j)].astype(jnp.float32)

    loop(0, chunks, project)

    if lines > 1:
        def add_parts(j):
            for r in range(1, lines):
                part_copy(r, j).wait_recv()
                acc[:, span(j)] += pin[lines - r - 1, :, span(j)].astype(jnp.float32)

        loop(0, chunks, add_parts)

    rounded = acc[...].astype(jnp.bfloat16)
    resid[...] = rounded
    widened = rounded.astype(jnp.float32)
    inv = lax.rsqrt(jnp.mean(widened * widened, axis=1, keepdims=True) + eps_norm)
    tokb[my_f] = (widened * inv * gain[...]).astype(jnp.bfloat16)

    def t_copy(f, j, way, target):
        at = tokb.at[f, :, span(j)]
        return copy(at, at, t_send.at[f, j, way], t_recv.at[f, j], target)

    def t_start(j, finish):
        for way, sign in ((0, 1), (1, -1)):
            to = my_f + sign

            @pl.when(inside(to, members))
            def _():
                mine = t_copy(my_f, j, way, dev(my_e, to))
                mine.wait_send() if finish else mine.start()

    def box_copy(f, e, j):
        return copy(outb.at[f, e, :, span(j)], inb.at[f, my_e, :, span(j)],
                    b_send.at[f, e], b_recv.at[f, my_e], dev(e, my_f))

    def box(f, j):
        boxed = lax.dot_general(mask[f, 0] + mask[f, 1], tokb[f, :, span(j)], TN,
                                preferred_element_type=jnp.float32).astype(jnp.bfloat16)
        for e in range(columns):
            outb[f, e, :, span(j)] = boxed[e * slots:(e + 1) * slots]
        loop(1, columns, lambda i: box_copy(f, lax.rem(my_e + i, columns), j).start())
        inb[f, my_e, :, span(j)] = outb[f, my_e, :, span(j)]

    def t_step(d, j, finish=False):
        for way, sign in ((0, 1), (1, -1)):
            fb, to = my_f - sign * d, my_f + sign

            @pl.when(inside(fb, members))
            def _():
                if not finish:
                    t_copy(fb, j, way, dev(my_e, my_f)).wait_recv()

                @pl.when(inside(to, members))
                def _():
                    onward = t_copy(fb, j, way, dev(my_e, to))
                    onward.wait_send() if finish else onward.start()

                if not finish:
                    box(fb, j)

    loop(0, chunks, lambda j: t_start(j, False))
    load_gu.wait()
    load_dn.wait()

    def back_copy(f, e, j):
        return copy(part.at[f, e, :, span(j)], back.at[f, my_e, :, span(j)],
                    r_send.at[f, e], r_recv.at[f, my_e, j], dev(e, my_f))

    def back_arrived(f, e, j):
        copy(part.at[f, e, :, span(j)], back.at[f, e, :, span(j)],
             r_send.at[f, e], r_recv.at[f, e, j], dev(e, my_f)).wait_recv()

    def expert(f):
        def boxes_arrived(i):
            e = lax.rem(my_e + i, columns)
            copy(outb.at[f, e], inb.at[f, e], b_send.at[f, e], b_recv.at[f, e], dev(e, my_f)).wait_recv()

        loop(1, columns, boxes_arrived)
        x = jnp.concatenate([inb[f, e] for e in range(columns)], axis=0)
        gate = lax.dot_general(x, gu[0], NT, preferred_element_type=jnp.float32)
        up = lax.dot_general(x, gu[1], NT, preferred_element_type=jnp.float32)
        hid[...] = (gate / (1.0 + jnp.exp(-gate)) * up).astype(jnp.bfloat16)

        def down(j):
            piece = jnp.dot(hid[...], dn[:, span(j)], preferred_element_type=jnp.float32).astype(jnp.bfloat16)
            for e in range(columns):
                part[f, e, :, span(j)] = piece[e * slots:(e + 1) * slots]
            loop(1, columns, lambda i: back_copy(f, lax.rem(my_e + i, columns), j).start())
            back[f, my_e, :, span(j)] = part[f, my_e, :, span(j)]

        loop(0, chunks, down)

        logits = lax.dot_general(tokb[f], router[...], NT, preferred_element_type=jnp.float32)
        s0 = jax.nn.sigmoid(jnp.sum(logits * hot[f, 0], axis=1, keepdims=True))
        s1 = jax.nn.sigmoid(jnp.sum(logits * hot[f, 1], axis=1, keepdims=True))
        weights = mask[f, 0].astype(jnp.float32) * (s0 / (s0 + s1)) + mask[f, 1].astype(jnp.float32) * (s1 / (s0 + s1))
        high = weights.astype(jnp.bfloat16)
        gates[f, 0] = high
        gates[f, 1] = (weights - high.astype(jnp.float32)).astype(jnp.bfloat16)

    def combine(f, j):
        loop(1, columns, lambda i: back_arrived(f, lax.rem(my_e + i, columns), j))
        results = jnp.concatenate([back[f, e, :, span(j)] for e in range(columns)], axis=0)
        return (jnp.dot(gates[f, 0], results, preferred_element_type=jnp.float32)
                + jnp.dot(gates[f, 1], results, preferred_element_type=jnp.float32))

    def sum_route(d, q):
        left = jnp.logical_xor(2 * my_f >= members, q == 1)
        f = jnp.where(left, members - 1 - d, d)
        active = jnp.where(left, my_f > f, my_f < f)
        outer = jnp.where(left, my_f < members - 1, my_f > 0)
        to = jnp.where(left, my_f - 1, my_f + 1)
        index = jnp.where(both(jnp.logical_not(left), to == f), members, f)
        return f, active, outer, jnp.clip(to, 0, members - 1), index

    def sum_copy(f, j, to, index):
        return copy(rs_out.at[f, :, span(j)], rs_in.at[index, :, span(j)],
                    s_send.at[f, j], s_recv.at[index, j], dev(my_e, to))

    def sum_arrived(index, j):
        at = rs_in.at[index, :, span(j)]
        copy(at, at, s_send.at[0, j], s_recv.at[index, j], dev(my_e, my_f)).wait_recv()

    def sum_step(d, i):
        j, q = lax.div(i, 2), lax.rem(i, 2)
        f, active, outer, to, index = sum_route(d, q)

        @pl.when(active)
        def _():
            total[...] = combine(f, j)

            @pl.when(outer)
            def _():
                sum_arrived(f, j)
                total[...] += rs_in[f, :, span(j)].astype(jnp.float32)

            rs_out[f, :, span(j)] = total[...].astype(jnp.bfloat16)
            sum_copy(f, j, to, index).start()

    shift = max(members - 3, 0)

    def slot(t):
        k, j = lax.div(t, chunks), lax.rem(t, chunks)

        @pl.when(k < members - 1)
        def _():
            t_step(k + 1, j)

        @pl.when(t == (members - 1) * chunks)
        def _():
            loop(0, chunks, lambda i: box(my_f, i))

        @pl.when(both(j == 0, both(k >= 1, k <= members)))
        def _():
            expert(group_of(lax.rem(k, members)))

        @pl.when(both(k > shift, k < members + shift))
        def _():
            loop(2 * j, 2 * j + 2, lambda i: sum_step(k - shift, i))

    loop(0, chunks * max(members + shift, members + 1), slot)

    def finish_own(j):
        total[...] = resid[:, span(j)].astype(jnp.float32) + combine(my_f, j)

        @pl.when(my_f < members - 1)
        def _():
            sum_arrived(my_f, j)
            total[...] += rs_in[my_f, :, span(j)].astype(jnp.float32)

        @pl.when(my_f > 0)
        def _():
            sum_arrived(members, j)
            total[...] += rs_in[members, :, span(j)].astype(jnp.float32)

        out[:, span(j)] = total[...].astype(jnp.bfloat16)

    loop(0, chunks, finish_own)

    def drain(j):
        w_start(j, True)
        t_start(j, True)
        loop(1, members, lambda s: w_step(s, j, True))
        loop(1, members, lambda d: t_step(d, j, True))
        for r in range(1, lines):
            part_copy(r, j).wait_send()

        def sums(i):
            f, active, outer, to, index = sum_route(lax.div(i, 2) + 1, lax.rem(i, 2))

            @pl.when(active)
            def _():
                sum_copy(f, j, to, index).wait_send()

        loop(0, 2 * (members - 1), sums)

    loop(0, chunks, drain)
    id_start(True)
    for r in range(1, lines):
        ctx_copy(r).wait_send()

    def drain_boxes(i):
        f, e = lax.div(i, columns), lax.rem(i, columns)

        @pl.when(e != my_e)
        def _():
            copy(outb.at[f, e], inb.at[f, my_e], b_send.at[f, e], b_recv.at[f, my_e], dev(e, my_f)).wait_send()
            copy(part.at[f, e], back.at[f, my_e], r_send.at[f, e], r_recv.at[f, my_e, 0], dev(e, my_f)).wait_send()

    loop(0, members * columns, drain_boxes)


def on_device(tokens, context, out_proj, norm_gain, router, expert_ids, w_gate_up, w_down):
    rows, width = tokens.shape
    columns = lax.axis_size("expert")
    members = lax.axis_size("fsdp")
    n = columns * members
    experts = n // 2
    lines = columns // 2
    cap = 5 * rows // (2 * experts)
    slots = -(-cap // 8) * 8
    units = w_down.shape[1]
    k_rows = out_proj.shape[0]
    col = min(512, width)
    chunks = width // col
    others = max(lines - 1, 1)
    vmem = pl.BlockSpec(memory_space=pltpu.VMEM)
    far = pl.BlockSpec(memory_space=pl.ANY)
    bf = jnp.bfloat16
    dma = pltpu.SemaphoreType.DMA
    boxes = pltpu.VMEM((members, columns, slots, width), bf)
    marks = pltpu.VMEM((members, 2, rows, columns * slots), bf)
    call = pl.pallas_call(
        functools.partial(block_kernel, columns, members, slots, col),
        out_shape=jax.ShapeDtypeStruct((rows, width), bf),
        in_specs=[vmem] * 6 + [far] * 2,
        out_specs=vmem,
        scratch_shapes=[
            pltpu.VMEM((2 * members * k_rows, width), bf),
            pltpu.VMEM((lines, rows, 2 * members * k_rows), bf),
            pltpu.VMEM((rows, width), jnp.float32),
            pltpu.VMEM((others, rows, width), bf),
            pltpu.VMEM((others, rows, width), bf),
            pltpu.VMEM((2, units, width), bf),
            pltpu.VMEM((units, width), bf),
            pltpu.VMEM((rows, width), bf),
            pltpu.VMEM((members, 2, rows), jnp.int32),
            pltpu.VMEM((members, 2, rows, experts), jnp.float32),
            marks,
            marks,
            pltpu.VMEM((members, rows, width), bf),
            boxes, boxes,
            pltpu.VMEM((columns * slots, units), bf),
            boxes, boxes,
            pltpu.VMEM((rows, col), jnp.float32),
            pltpu.VMEM((members, rows, width), bf),
            pltpu.VMEM((members + 1, rows, width), bf),
            dma((2,)), dma((members, chunks, 3)), dma((2, members, chunks)),
            dma((members, 2)), dma((members,)), dma((lines,)), dma((lines,)),
            dma((others, chunks)), dma((others, chunks)),
            dma((members, chunks, 2)), dma((members, chunks)),
            dma((members, columns)), dma((members, columns)),
            dma((members, columns)), dma((members, columns, chunks)),
            dma((members, chunks)), dma((members + 1, chunks)),
        ],
        compiler_params=pltpu.CompilerParams(
            collective_id=0, has_side_effects=True, vmem_limit_bytes=VMEM_GRANT),
    )
    return call(tokens, context, out_proj, norm_gain.reshape(1, width), router.T, expert_ids.T, w_gate_up, w_down)


def solution(mesh):
    group = ("sweep", "expert", "fsdp")
    return jax.shard_map(
        on_device,
        mesh=mesh,
        in_specs=(
            P(group, None), P(group, None), P(group, None), P("sweep"), P("sweep", None),
            P(group, None), P(group, None, None, None), P(group, None, None),
        ),
        out_specs=P(group, None),
        check_vma=False,
    )
```

```python
import functools

import jax
import jax.numpy as jnp
from jax import lax
from jax.experimental import pallas as pl
from jax.experimental.pallas import tpu as pltpu
from jax.sharding import PartitionSpec as P

eps_norm = 1e-05
MESH = pl.DeviceIdType.MESH
VMEM_GRANT = 62 * 1024 * 1024
NT = (((1,), (1,)), ((), ()))
TN = (((0,), (0,)), ((), ()))


def both(a, b):
    return jnp.logical_and(a, b)


def inside(i, n):
    return both(i >= 0, i < n)


def block_kernel(
    columns, members, slots, col,
    tok, ctx, wout, gain, router, ids, gu_hbm, dn_hbm,
    out,
    gath, ctxs, acc, pout, pin, gu, dn, resid,
    idsb, hot, mask, gates, tokb, outb, inb, hid, part, back, total, rs_out, rs_in,
    load_sem, w_send, w_recv, id_send, id_recv, c_send, c_recv, p_send, p_recv,
    t_send, t_recv, b_send, b_recv, r_send, r_recv, s_send, s_recv,
):
    lines = columns // 2
    pairs = members // 2
    experts = columns * pairs
    rows, width = tok.shape
    k_rows = wout.shape[0]
    depth = 2 * members * k_rows
    chunks = width // col
    my_e = lax.axis_index("expert")
    my_f = lax.axis_index("fsdp")
    my_y, my_c = lax.div(my_e, 2), lax.rem(my_e, 2)
    my_p = lax.div(my_f, 2)
    other = my_y * 2 + 1 - my_c

    def dev(e, f):
        return {"expert": e, "fsdp": f}

    def span(j):
        return pl.ds(pl.multiple_of(j * col, col), col)

    def copy(src, dst, send, recv, target):
        return pltpu.make_async_remote_copy(
            src_ref=src, dst_ref=dst, send_sem=send, recv_sem=recv,
            device_id=target, device_id_type=MESH)

    def loop(lo, hi, body):
        def one(i, _):
            body(i)
            return 0

        lax.fori_loop(lo, hi, one, 0)

    load_gu = pltpu.make_async_copy(gu_hbm.at[0], gu, load_sem.at[0])
    load_dn = pltpu.make_async_copy(dn_hbm.at[0], dn, load_sem.at[1])

    barrier = pltpu.get_barrier_semaphore()

    def greet(e, f):
        pl.semaphore_signal(barrier, inc=1, device_id=dev(e, f), device_id_type=MESH)

    for sign in (1, -1):
        @pl.when(inside(my_f + sign, members))
        def _():
            greet(my_e, my_f + sign)

    loop(1, columns, lambda i: greet(lax.rem(my_e + i, columns), my_f))
    beside = jnp.where(my_f > 0, 1, 0) + jnp.where(my_f < members - 1, 1, 0)
    pl.semaphore_wait(barrier, columns - 1 + beside)

    def place(c, f):
        return pl.ds(pl.multiple_of((c * members + f) * k_rows, k_rows), k_rows)

    def w_copy(f, j, way, target, own=False):
        at = gath.at[place(my_c, f), span(j)]
        return copy(wout.at[:, span(j)] if own else at, at,
                    w_send.at[f, j, way], w_recv.at[my_c, f, j], target)

    def w_arrived(c, f, j):
        at = gath.at[place(c, f), span(j)]
        copy(at, at, w_send.at[f, j, 0], w_recv.at[c, f, j], dev(other, my_f)).wait_recv()

    def id_copy(f, way, target, own=False):
        return copy(ids if own else idsb.at[f], idsb.at[f], id_send.at[f, way], id_recv.at[f], target)

    def ctx_copy(r):
        line = lax.rem(my_y + r, lines)
        at = pl.ds(pl.multiple_of(line * depth, depth), depth)
        return copy(ctx.at[:, at], ctxs.at[lines - r], c_send.at[r], c_recv.at[lines - r],
                    dev(line * 2 + my_c, my_f))

    def w_start(j, finish):
        for way, sign in ((0, 1), (1, -1)):
            to = my_f + sign

            @pl.when(inside(to, members))
            def _():
                mine = w_copy(my_f, j, way, dev(my_e, to), True)
                mine.wait_send() if finish else mine.start()
        mine = w_copy(my_f, j, 2, dev(other, my_f), True)
        mine.wait_send() if finish else mine.start()

    def id_start(finish):
        for way, sign in ((0, 1), (1, -1)):
            to = my_f + sign

            @pl.when(inside(to, members))
            def _():
                mine = id_copy(my_f, way, dev(my_e, to), True)
                mine.wait_send() if finish else mine.start()

    def w_step(s, j, finish=False):
        for way, sign in ((0, 1), (1, -1)):
            fb, to = my_f - sign * s, my_f + sign

            @pl.when(inside(fb, members))
            def _():
                if not finish:
                    w_arrived(my_c, fb, j)

                    @pl.when(j == 0)
                    def _():
                        id_copy(fb, way, dev(my_e, my_f)).wait_recv()

                @pl.when(inside(to, members))
                def _():
                    onward = w_copy(fb, j, way, dev(my_e, to))
                    onward.wait_send() if finish else onward.start()

                    @pl.when(j == 0)
                    def _():
                        named = id_copy(fb, way, dev(my_e, to))
                        named.wait_send() if finish else named.start()

                across = w_copy(fb, j, 2, dev(other, my_f))
                across.wait_send() if finish else across.start()

    loop(0, chunks, lambda j: w_start(j, False))
    id_start(False)
    for r in range(1, lines):
        ctx_copy(r).start()
    load_gu.start()
    load_dn.start()
    loop(0, chunks, lambda j: gath.__setitem__((place(my_c, my_f), span(j)), wout[:, span(j)]))
    idsb[my_f] = ids[...]
    ctxs[0] = ctx[:, pl.ds(pl.multiple_of(my_y * depth, depth), depth)]
    loop(0, (members - 2) * chunks, lambda i: w_step(1 + lax.div(i, chunks), lax.rem(i, chunks)))
    for r in range(1, lines):
        ctx_copy(r).wait_recv()

    def group_of(k):
        m = jnp.minimum(my_f, members - 1 - my_f)
        half = lax.div(k + 1, 2)
        near = jnp.where(lax.rem(k, 2) == 1, my_f - half, my_f + half)
        far = jnp.where(my_f > m, my_f - (k - m), my_f + (k - m))
        return jnp.where(k <= 2 * m, near, far)

    def make_masks(f):
        diagonal = jnp.where(
            lax.broadcasted_iota(jnp.int32, (rows, rows), 0) == lax.broadcasted_iota(jnp.int32, (rows, rows), 1),
            1.0, 0.0)
        names = idsb[f].astype(jnp.float32)
        id0 = jnp.sum(diagonal * names[0:1], axis=1, keepdims=True).astype(jnp.int32)
        id1 = jnp.sum(diagonal * names[1:2], axis=1, keepdims=True).astype(jnp.int32)
        every = lax.broadcasted_iota(jnp.int32, (rows, experts), 1)
        hot[f, 0] = jnp.where(every == id0, 1.0, 0.0)
        hot[f, 1] = jnp.where(every == id1, 1.0, 0.0)
        place_no = lax.broadcasted_iota(jnp.int32, (rows, columns), 1)
        here = place_no * pairs + my_p
        hot0 = jnp.where(here == id0, 1.0, 0.0)
        hot1 = jnp.where(here == id1, 1.0, 0.0)
        earlier = jnp.where(
            lax.broadcasted_iota(jnp.int32, (rows, rows), 1) < lax.broadcasted_iota(jnp.int32, (rows, rows), 0),
            1.0, 0.0).astype(jnp.bfloat16)
        before = jnp.dot(earlier, (hot0 + hot1).astype(jnp.bfloat16), preferred_element_type=jnp.float32)
        spot = before + (place_no * slots + 1).astype(jnp.float32)
        slot0 = jnp.sum(spot * hot0, axis=1, keepdims=True).astype(jnp.int32) - 1
        slot1 = jnp.sum(spot * hot1, axis=1, keepdims=True).astype(jnp.int32) - 1
        slot_no = lax.broadcasted_iota(jnp.int32, (rows, columns * slots), 1)
        mask[f, 0] = jnp.where(slot_no == slot0, 1.0, 0.0).astype(jnp.bfloat16)
        mask[f, 1] = jnp.where(slot_no == slot1, 1.0, 0.0).astype(jnp.bfloat16)

    def part_copy(r, j):
        line = lax.rem(my_y + r, lines)
        return copy(pout.at[r - 1, :, span(j)], pin.at[lines - r - 1, :, span(j)],
                    p_send.at[r - 1, j], p_recv.at[lines - r - 1, j], dev(line * 2 + my_c, my_f))

    def project(j):
        loop(lax.div(j * members, chunks), lax.div((j + 1) * members, chunks),
             lambda k: make_masks(group_of(k)))
        w_step(members - 1, j)
        loop(0, members, lambda f: w_arrived(1 - my_c, f, j))
        mixed = jnp.dot(ctxs[...].reshape(lines * rows, depth), gath[:, span(j)],
                        preferred_element_type=jnp.float32)
        for r in range(1, lines):
            pout[r - 1, :, span(j)] = mixed[r * rows:(r + 1) * rows].astype(jnp.bfloat16)
            part_copy(r, j).start()
        acc[:, span(j)] = mixed[:rows] + tok[:, span(j)].astype(jnp.float32)

    loop(0, chunks, project)

    if lines > 1:
        def add_parts(j):
            for r in range(1, lines):
                part_copy(r, j).wait_recv()
                acc[:, span(j)] += pin[lines - r - 1, :, span(j)].astype(jnp.float32)

        loop(0, chunks, add_parts)

    rounded = acc[...].astype(jnp.bfloat16)
    resid[...] = rounded
    widened = rounded.astype(jnp.float32)
    inv = lax.rsqrt(jnp.mean(widened * widened, axis=1, keepdims=True) + eps_norm)
    tokb[my_f] = (widened * inv * gain[...]).astype(jnp.bfloat16)

    def t_copy(f, j, way, target):
        at = tokb.at[f, :, span(j)]
        return copy(at, at, t_send.at[f, j, way], t_recv.at[f, j], target)

    def t_start(j, finish):
        for way, sign in ((0, 1), (1, -1)):
            to = my_f + sign

            @pl.when(inside(to, members))
            def _():
                mine = t_copy(my_f, j, way, dev(my_e, to))
                mine.wait_send() if finish else mine.start()

    def box_copy(f, e, j):
        return copy(outb.at[f, e, :, span(j)], inb.at[f, my_e, :, span(j)],
                    b_send.at[f, e], b_recv.at[f, my_e], dev(e, my_f))

    def box(f, j):
        boxed = lax.dot_general(mask[f, 0] + mask[f, 1], tokb[f, :, span(j)], TN,
                                preferred_element_type=jnp.float32).astype(jnp.bfloat16)
        for e in range(columns):
            outb[f, e, :, span(j)] = boxed[e * slots:(e + 1) * slots]
        loop(1, columns, lambda i: box_copy(f, lax.rem(my_e + i, columns), j).start())
        inb[f, my_e, :, span(j)] = outb[f, my_e, :, span(j)]

    def t_step(d, j, finish=False):
        for way, sign in ((0, 1), (1, -1)):
            fb, to = my_f - sign * d, my_f + sign

            @pl.when(inside(fb, members))
            def _():
                if not finish:
                    t_copy(fb, j, way, dev(my_e, my_f)).wait_recv()

                @pl.when(inside(to, members))
                def _():
                    onward = t_copy(fb, j, way, dev(my_e, to))
                    onward.wait_send() if finish else onward.start()

                if not finish:
                    box(fb, j)

    loop(0, chunks, lambda j: t_start(j, False))
    load_gu.wait()
    load_dn.wait()

    def back_copy(f, e, j):
        return copy(part.at[f, e, :, span(j)], back.at[f, my_e, :, span(j)],
                    r_send.at[f, e], r_recv.at[f, my_e, j], dev(e, my_f))

    def back_arrived(f, e, j):
        copy(part.at[f, e, :, span(j)], back.at[f, e, :, span(j)],
             r_send.at[f, e], r_recv.at[f, e, j], dev(e, my_f)).wait_recv()

    def expert(f):
        def boxes_arrived(i):
            e = lax.rem(my_e + i, columns)
            copy(outb.at[f, e], inb.at[f, e], b_send.at[f, e], b_recv.at[f, e], dev(e, my_f)).wait_recv()

        loop(1, columns, boxes_arrived)
        x = jnp.concatenate([inb[f, e] for e in range(columns)], axis=0)
        gate = lax.dot_general(x, gu[0], NT, preferred_element_type=jnp.float32)
        up = lax.dot_general(x, gu[1], NT, preferred_element_type=jnp.float32)
        hid[...] = (gate / (1.0 + jnp.exp(-gate)) * up).astype(jnp.bfloat16)

        def down(j):
            piece = jnp.dot(hid[...], dn[:, span(j)], preferred_element_type=jnp.float32).astype(jnp.bfloat16)
            for e in range(columns):
                part[f, e, :, span(j)] = piece[e * slots:(e + 1) * slots]
            loop(1, columns, lambda i: back_copy(f, lax.rem(my_e + i, columns), j).start())
            back[f, my_e, :, span(j)] = part[f, my_e, :, span(j)]

        loop(0, chunks, down)

        logits = lax.dot_general(tokb[f], router[...], NT, preferred_element_type=jnp.float32)
        s0 = jax.nn.sigmoid(jnp.sum(logits * hot[f, 0], axis=1, keepdims=True))
        s1 = jax.nn.sigmoid(jnp.sum(logits * hot[f, 1], axis=1, keepdims=True))
        weights = mask[f, 0].astype(jnp.float32) * (s0 / (s0 + s1)) + mask[f, 1].astype(jnp.float32) * (s1 / (s0 + s1))
        high = weights.astype(jnp.bfloat16)
        gates[f, 0] = high
        gates[f, 1] = (weights - high.astype(jnp.float32)).astype(jnp.bfloat16)

    def combine(f, j):
        loop(1, columns, lambda i: back_arrived(f, lax.rem(my_e + i, columns), j))
        results = jnp.concatenate([back[f, e, :, span(j)] for e in range(columns)], axis=0)
        return (jnp.dot(gates[f, 0], results, preferred_element_type=jnp.float32)
                + jnp.dot(gates[f, 1], results, preferred_element_type=jnp.float32))

    def sum_route(d, q):
        left = jnp.logical_xor(2 * my_f >= members, q == 1)
        f = jnp.where(left, members - 1 - d, d)
        active = jnp.where(left, my_f > f, my_f < f)
        outer = jnp.where(left, my_f < members - 1, my_f > 0)
        to = jnp.where(left, my_f - 1, my_f + 1)
        index = jnp.where(both(jnp.logical_not(left), to == f), members, f)
        return f, active, outer, jnp.clip(to, 0, members - 1), index

    def sum_copy(f, j, to, index):
        return copy(rs_out.at[f, :, span(j)], rs_in.at[index, :, span(j)],
                    s_send.at[f, j], s_recv.at[index, j], dev(my_e, to))

    def sum_arrived(index, j):
        at = rs_in.at[index, :, span(j)]
        copy(at, at, s_send.at[0, j], s_recv.at[index, j], dev(my_e, my_f)).wait_recv()

    def sum_step(d, j, q):
        f, active, outer, to, index = sum_route(d, q)

        @pl.when(active)
        def _():
            total[...] = combine(f, j)

            @pl.when(outer)
            def _():
                sum_arrived(f, j)
                total[...] += rs_in[f, :, span(j)].astype(jnp.float32)

            rs_out[f, :, span(j)] = total[...].astype(jnp.bfloat16)
            sum_copy(f, j, to, index).start()

    def sum_steps(d):
        def one(i):
            @pl.when(i < chunks)
            def _():
                sum_step(d, i, 0)

            @pl.when(i > 0)
            def _():
                sum_step(d, i - 1, 1)

        loop(0, chunks + 1, one)

    shift = max(members - 3, 0)
    at_end = jnp.logical_or(my_f == 0, my_f == members - 1)

    def slot(t):
        k, j = lax.div(t, chunks), lax.rem(t, chunks)
        summing = both(k > shift, k < members + shift)

        @pl.when(k < members - 1)
        def _():
            t_step(k + 1, j)

        @pl.when(t == (members - 1) * chunks)
        def _():
            loop(0, chunks, lambda i: box(my_f, i))

        @pl.when(both(summing, both(at_end, j == 0)))
        def _():
            sum_steps(k - shift)

        @pl.when(both(j == 0, both(k >= 1, k <= members)))
        def _():
            expert(group_of(lax.rem(k, members)))

        @pl.when(both(summing, both(jnp.logical_not(at_end), j == 1)))
        def _():
            sum_steps(k - shift)

    loop(0, chunks * max(members + shift, members + 1), slot)

    def finish_own(j):
        total[...] = resid[:, span(j)].astype(jnp.float32) + combine(my_f, j)

        @pl.when(my_f < members - 1)
        def _():
            sum_arrived(my_f, j)
            total[...] += rs_in[my_f, :, span(j)].astype(jnp.float32)

        @pl.when(my_f > 0)
        def _():
            sum_arrived(members, j)
            total[...] += rs_in[members, :, span(j)].astype(jnp.float32)

        out[:, span(j)] = total[...].astype(jnp.bfloat16)

    loop(0, chunks, finish_own)

    def drain(j):
        w_start(j, True)
        t_start(j, True)
        loop(1, members, lambda s: w_step(s, j, True))
        loop(1, members, lambda d: t_step(d, j, True))
        for r in range(1, lines):
            part_copy(r, j).wait_send()

        def sums(i):
            f, active, outer, to, index = sum_route(lax.div(i, 2) + 1, lax.rem(i, 2))

            @pl.when(active)
            def _():
                sum_copy(f, j, to, index).wait_send()

        loop(0, 2 * (members - 1), sums)

    loop(0, chunks, drain)
    id_start(True)
    for r in range(1, lines):
        ctx_copy(r).wait_send()

    def drain_boxes(i):
        f, e = lax.div(i, columns), lax.rem(i, columns)

        @pl.when(e != my_e)
        def _():
            copy(outb.at[f, e], inb.at[f, my_e], b_send.at[f, e], b_recv.at[f, my_e], dev(e, my_f)).wait_send()
            copy(part.at[f, e], back.at[f, my_e], r_send.at[f, e], r_recv.at[f, my_e, 0], dev(e, my_f)).wait_send()

    loop(0, members * columns, drain_boxes)


def on_device(tokens, context, out_proj, norm_gain, router, expert_ids, w_gate_up, w_down):
    rows, width = tokens.shape
    columns = lax.axis_size("expert")
    members = lax.axis_size("fsdp")
    n = columns * members
    experts = n // 2
    lines = columns // 2
    cap = 5 * rows // (2 * experts)
    slots = -(-cap // 8) * 8
    units = w_down.shape[1]
    k_rows = out_proj.shape[0]
    col = min(512, width)
    chunks = width // col
    others = max(lines - 1, 1)
    vmem = pl.BlockSpec(memory_space=pltpu.VMEM)
    far = pl.BlockSpec(memory_space=pl.ANY)
    bf = jnp.bfloat16
    dma = pltpu.SemaphoreType.DMA
    boxes = pltpu.VMEM((members, columns, slots, width), bf)
    marks = pltpu.VMEM((members, 2, rows, columns * slots), bf)
    call = pl.pallas_call(
        functools.partial(block_kernel, columns, members, slots, col),
        out_shape=jax.ShapeDtypeStruct((rows, width), bf),
        in_specs=[vmem] * 6 + [far] * 2,
        out_specs=vmem,
        scratch_shapes=[
            pltpu.VMEM((2 * members * k_rows, width), bf),
            pltpu.VMEM((lines, rows, 2 * members * k_rows), bf),
            pltpu.VMEM((rows, width), jnp.float32),
            pltpu.VMEM((others, rows, width), bf),
            pltpu.VMEM((others, rows, width), bf),
            pltpu.VMEM((2, units, width), bf),
            pltpu.VMEM((units, width), bf),
            pltpu.VMEM((rows, width), bf),
            pltpu.VMEM((members, 2, rows), jnp.int32),
            pltpu.VMEM((members, 2, rows, experts), jnp.float32),
            marks,
            marks,
            pltpu.VMEM((members, rows, width), bf),
            boxes, boxes,
            pltpu.VMEM((columns * slots, units), bf),
            boxes, boxes,
            pltpu.VMEM((rows, col), jnp.float32),
            pltpu.VMEM((members, rows, width), bf),
            pltpu.VMEM((members + 1, rows, width), bf),
            dma((2,)), dma((members, chunks, 3)), dma((2, members, chunks)),
            dma((members, 2)), dma((members,)), dma((lines,)), dma((lines,)),
            dma((others, chunks)), dma((others, chunks)),
            dma((members, chunks, 2)), dma((members, chunks)),
            dma((members, columns)), dma((members, columns)),
            dma((members, columns)), dma((members, columns, chunks)),
            dma((members, chunks)), dma((members + 1, chunks)),
        ],
        compiler_params=pltpu.CompilerParams(
            collective_id=0, has_side_effects=True, vmem_limit_bytes=VMEM_GRANT),
    )
    return call(tokens, context, out_proj, norm_gain.reshape(1, width), router.T, expert_ids.T, w_gate_up, w_down)


def solution(mesh):
    group = ("sweep", "expert", "fsdp")
    return jax.shard_map(
        on_device,
        mesh=mesh,
        in_specs=(
            P(group, None), P(group, None), P(group, None), P("sweep"), P("sweep", None),
            P(group, None), P(group, None, None, None), P(group, None, None),
        ),
        out_specs=P(group, None),
        check_vma=False,
    )
```

```python
import functools

import jax
import jax.numpy as jnp
from jax import lax
from jax.experimental import pallas as pl
from jax.experimental.pallas import tpu as pltpu
from jax.sharding import PartitionSpec as P

eps_norm = 1e-05
MESH = pl.DeviceIdType.MESH
VMEM_GRANT = 62 * 1024 * 1024
NT = (((1,), (1,)), ((), ()))
TN = (((0,), (0,)), ((), ()))


def both(a, b):
    return jnp.logical_and(a, b)


def inside(i, n):
    return both(i >= 0, i < n)


def block_kernel(
    columns, members, slots, col,
    tok, ctx, wout, gain, router, ids, gu_hbm, dn_hbm,
    out,
    gath, ctxs, acc, pout, pin, gu, dn, resid,
    idsb, hot, mask, gates, tokb, outb, inb, hid, part, back, given, total, rs_out, rs_in,
    load_sem, w_send, w_recv, id_send, id_recv, c_send, c_recv, p_send, p_recv,
    t_send, t_recv, b_send, b_recv, r_send, r_recv, g_send, g_recv, s_send, s_recv,
):
    lines = columns // 2
    pairs = members // 2
    experts = columns * pairs
    rows, width = tok.shape
    k_rows = wout.shape[0]
    depth = 2 * members * k_rows
    chunks = width // col
    my_e = lax.axis_index("expert")
    my_f = lax.axis_index("fsdp")
    my_y, my_c = lax.div(my_e, 2), lax.rem(my_e, 2)
    my_p = lax.div(my_f, 2)
    other = my_y * 2 + 1 - my_c
    half_f = my_f + 1 - 2 * lax.rem(my_f, 2)

    def dev(e, f):
        return {"expert": e, "fsdp": f}

    def span(j):
        return pl.ds(pl.multiple_of(j * col, col), col)

    def copy(src, dst, send, recv, target):
        return pltpu.make_async_remote_copy(
            src_ref=src, dst_ref=dst, send_sem=send, recv_sem=recv,
            device_id=target, device_id_type=MESH)

    def loop(lo, hi, body):
        def one(i, _):
            body(i)
            return 0

        lax.fori_loop(lo, hi, one, 0)

    load_gu = pltpu.make_async_copy(gu_hbm.at[0], gu, load_sem.at[0])
    load_dn = pltpu.make_async_copy(dn_hbm.at[0], dn, load_sem.at[1])

    barrier = pltpu.get_barrier_semaphore()

    def greet(e, f):
        pl.semaphore_signal(barrier, inc=1, device_id=dev(e, f), device_id_type=MESH)

    for sign in (1, -1):
        @pl.when(inside(my_f + sign, members))
        def _():
            greet(my_e, my_f + sign)

    loop(1, columns, lambda i: greet(lax.rem(my_e + i, columns), my_f))
    beside = jnp.where(my_f > 0, 1, 0) + jnp.where(my_f < members - 1, 1, 0)
    pl.semaphore_wait(barrier, columns - 1 + beside)

    def place(c, f):
        return pl.ds(pl.multiple_of((c * members + f) * k_rows, k_rows), k_rows)

    def w_copy(f, j, way, target, own=False):
        at = gath.at[place(my_c, f), span(j)]
        return copy(wout.at[:, span(j)] if own else at, at,
                    w_send.at[f, j, way], w_recv.at[my_c, f, j], target)

    def w_arrived(c, f, j):
        at = gath.at[place(c, f), span(j)]
        copy(at, at, w_send.at[f, j, 0], w_recv.at[c, f, j], dev(other, my_f)).wait_recv()

    def id_copy(f, way, target, own=False):
        return copy(ids if own else idsb.at[f], idsb.at[f], id_send.at[f, way], id_recv.at[f], target)

    def ctx_copy(r):
        line = lax.rem(my_y + r, lines)
        at = pl.ds(pl.multiple_of(line * depth, depth), depth)
        return copy(ctx.at[:, at], ctxs.at[lines - r], c_send.at[r], c_recv.at[lines - r],
                    dev(line * 2 + my_c, my_f))

    def w_start(j, finish):
        for way, sign in ((0, 1), (1, -1)):
            to = my_f + sign

            @pl.when(inside(to, members))
            def _():
                mine = w_copy(my_f, j, way, dev(my_e, to), True)
                mine.wait_send() if finish else mine.start()
        mine = w_copy(my_f, j, 2, dev(other, my_f), True)
        mine.wait_send() if finish else mine.start()

    def id_start(finish):
        for way, sign in ((0, 1), (1, -1)):
            to = my_f + sign

            @pl.when(inside(to, members))
            def _():
                mine = id_copy(my_f, way, dev(my_e, to), True)
                mine.wait_send() if finish else mine.start()

    def w_step(s, j, finish=False):
        for way, sign in ((0, 1), (1, -1)):
            fb, to = my_f - sign * s, my_f + sign

            @pl.when(inside(fb, members))
            def _():
                if not finish:
                    w_arrived(my_c, fb, j)

                    @pl.when(j == 0)
                    def _():
                        id_copy(fb, way, dev(my_e, my_f)).wait_recv()

                @pl.when(inside(to, members))
                def _():
                    onward = w_copy(fb, j, way, dev(my_e, to))
                    onward.wait_send() if finish else onward.start()

                    @pl.when(j == 0)
                    def _():
                        named = id_copy(fb, way, dev(my_e, to))
                        named.wait_send() if finish else named.start()

                across = w_copy(fb, j, 2, dev(other, my_f))
                across.wait_send() if finish else across.start()

    loop(0, chunks, lambda j: w_start(j, False))
    id_start(False)
    for r in range(1, lines):
        ctx_copy(r).start()
    load_gu.start()
    load_dn.start()
    loop(0, chunks, lambda j: gath.__setitem__((place(my_c, my_f), span(j)), wout[:, span(j)]))
    idsb[my_f] = ids[...]
    ctxs[0] = ctx[:, pl.ds(pl.multiple_of(my_y * depth, depth), depth)]
    inner = jnp.where(2 * my_f >= members, -1, 1)

    def group_of(k):
        m = jnp.minimum(my_f, members - 1 - my_f)
        half = lax.div(k + 1, 2)
        near = jnp.where(lax.rem(k, 2) == 1, my_f + inner * half, my_f - inner * half)
        return jnp.where(k <= 2 * m, near, my_f + inner * (k - m))

    def make_masks(f):
        diagonal = jnp.where(
            lax.broadcasted_iota(jnp.int32, (rows, rows), 0) == lax.broadcasted_iota(jnp.int32, (rows, rows), 1),
            1.0, 0.0)
        names = idsb[f].astype(jnp.float32)
        id0 = jnp.sum(diagonal * names[0:1], axis=1, keepdims=True).astype(jnp.int32)
        id1 = jnp.sum(diagonal * names[1:2], axis=1, keepdims=True).astype(jnp.int32)
        every = lax.broadcasted_iota(jnp.int32, (rows, experts), 1)
        hot[f, 0] = jnp.where(every == id0, 1.0, 0.0)
        hot[f, 1] = jnp.where(every == id1, 1.0, 0.0)
        place_no = lax.broadcasted_iota(jnp.int32, (rows, columns), 1)
        here = place_no * pairs + my_p
        hot0 = jnp.where(here == id0, 1.0, 0.0)
        hot1 = jnp.where(here == id1, 1.0, 0.0)
        earlier = jnp.where(
            lax.broadcasted_iota(jnp.int32, (rows, rows), 1) < lax.broadcasted_iota(jnp.int32, (rows, rows), 0),
            1.0, 0.0).astype(jnp.bfloat16)
        before = jnp.dot(earlier, (hot0 + hot1).astype(jnp.bfloat16), preferred_element_type=jnp.float32)
        spot = before + (place_no * slots + 1).astype(jnp.float32)
        slot0 = jnp.sum(spot * hot0, axis=1, keepdims=True).astype(jnp.int32) - 1
        slot1 = jnp.sum(spot * hot1, axis=1, keepdims=True).astype(jnp.int32) - 1
        slot_no = lax.broadcasted_iota(jnp.int32, (rows, columns * slots), 1)
        mask[f, 0] = jnp.where(slot_no == slot0, 1.0, 0.0).astype(jnp.bfloat16)
        mask[f, 1] = jnp.where(slot_no == slot1, 1.0, 0.0).astype(jnp.bfloat16)

    def part_copy(r, j):
        line = lax.rem(my_y + r, lines)
        return copy(pout.at[r - 1, :, span(j)], pin.at[lines - r - 1, :, span(j)],
                    p_send.at[r - 1, j], p_recv.at[lines - r - 1, j], dev(line * 2 + my_c, my_f))

    def project(j):
        loop(0, members, lambda f: w_arrived(1 - my_c, f, j))
        mixed = jnp.dot(ctxs[...].reshape(lines * rows, depth), gath[:, span(j)],
                        preferred_element_type=jnp.float32)
        for r in range(1, lines):
            pout[r - 1, :, span(j)] = mixed[r * rows:(r + 1) * rows].astype(jnp.bfloat16)
            part_copy(r, j).start()
        acc[:, span(j)] = mixed[:rows] + tok[:, span(j)].astype(jnp.float32)

    farthest = jnp.maximum(my_f, members - 1 - my_f)

    def gather(i):
        s, j = 1 + lax.div(i, chunks), lax.rem(i, chunks)

        @pl.when(s == farthest)
        def _():
            @pl.when(j == 0)
            def _():
                for r in range(1, lines):
                    ctx_copy(r).wait_recv()

            loop(lax.div(j * members, chunks), lax.div((j + 1) * members, chunks),
                 lambda k: make_masks(group_of(k)))

        w_step(s, j)

        @pl.when(s == farthest)
        def _():
            project(j)

    loop(0, (members - 1) * chunks, gather)

    if lines > 1:
        def add_parts(j):
            for r in range(1, lines):
                part_copy(r, j).wait_recv()
                acc[:, span(j)] += pin[lines - r - 1, :, span(j)].astype(jnp.float32)

        loop(0, chunks, add_parts)

    rounded = acc[...].astype(jnp.bfloat16)
    resid[...] = rounded
    widened = rounded.astype(jnp.float32)
    inv = lax.rsqrt(jnp.mean(widened * widened, axis=1, keepdims=True) + eps_norm)
    tokb[my_f] = (widened * inv * gain[...]).astype(jnp.bfloat16)

    def t_copy(f, j, way, target):
        at = tokb.at[f, :, span(j)]
        return copy(at, at, t_send.at[f, j, way], t_recv.at[f, j], target)

    def t_start(j, finish):
        for way, sign in ((0, 1), (1, -1)):
            to = my_f + sign

            @pl.when(inside(to, members))
            def _():
                mine = t_copy(my_f, j, way, dev(my_e, to))
                mine.wait_send() if finish else mine.start()

    def box_copy(f, e, j):
        return copy(outb.at[f, e, :, span(j)], inb.at[f, my_e, :, span(j)],
                    b_send.at[f, e], b_recv.at[f, my_e], dev(e, my_f))

    def box(f, j):
        boxed = lax.dot_general(mask[f, 0] + mask[f, 1], tokb[f, :, span(j)], TN,
                                preferred_element_type=jnp.float32).astype(jnp.bfloat16)
        for e in range(columns):
            outb[f, e, :, span(j)] = boxed[e * slots:(e + 1) * slots]
        loop(1, columns, lambda i: box_copy(f, lax.rem(my_e + i, columns), j).start())
        inb[f, my_e, :, span(j)] = outb[f, my_e, :, span(j)]

    def t_step(k, j, finish=False):
        f = group_of(k)
        step = jnp.where(f < my_f, 1, -1)
        to = my_f + step
        onward = t_copy(f, j, 0, dev(my_e, jnp.clip(to, 0, members - 1)))
        if not finish:
            onward.wait_recv()

        @pl.when(inside(to, members))
        def _():
            onward.wait_send() if finish else onward.start()

        if not finish:
            box(f, j)

    loop(0, chunks, lambda j: t_start(j, False))
    nothing = jnp.zeros((slots, width), jnp.bfloat16)
    loop(2, columns, lambda i: back.__setitem__((half_f, lax.rem(my_y * 2 + i, columns)), nothing))
    load_gu.wait()
    load_dn.wait()

    def back_copy(f, e, j):
        return copy(part.at[f, e, :, span(j)], back.at[f, my_e, :, span(j)],
                    r_send.at[f, e], r_recv.at[f, my_e, j], dev(e, my_f))

    def back_arrived(f, e, j):
        copy(part.at[f, e, :, span(j)], back.at[f, e, :, span(j)],
             r_send.at[f, e], r_recv.at[f, e, j], dev(e, my_f)).wait_recv()


    def give(e, j):
        return copy(part.at[half_f, e, :, span(j)], given.at[e, :, span(j)],
                    g_send.at[e, j], g_recv.at[e, j], dev(my_e, half_f))

    def expert(f):
        def boxes_arrived(i):
            e = lax.rem(my_e + i, columns)
            copy(outb.at[f, e], inb.at[f, e], b_send.at[f, e], b_recv.at[f, e], dev(e, my_f)).wait_recv()

        loop(1, columns, boxes_arrived)
        x = jnp.concatenate([inb[f, e] for e in range(columns)], axis=0)
        gate = lax.dot_general(x, gu[0], NT, preferred_element_type=jnp.float32)
        up = lax.dot_general(x, gu[1], NT, preferred_element_type=jnp.float32)
        hid[...] = (gate / (1.0 + jnp.exp(-gate)) * up).astype(jnp.bfloat16)

        def down(j):
            piece = jnp.dot(hid[...], dn[:, span(j)], preferred_element_type=jnp.float32).astype(jnp.bfloat16)
            for e in range(columns):
                part[f, e, :, span(j)] = piece[e * slots:(e + 1) * slots]
            back_copy(f, other, j).start()
            back[f, my_e, :, span(j)] = part[f, my_e, :, span(j)]

            def far_line(i):
                e = lax.rem(my_y * 2 + i, columns)

                @pl.when(f == half_f)
                def _():
                    give(e, j).start()

                @pl.when(f == my_f)
                def _():
                    give(e, j).wait_recv()
                    part[f, e, :, span(j)] = (part[f, e, :, span(j)].astype(jnp.float32)
                                              + given[e, :, span(j)].astype(jnp.float32)).astype(jnp.bfloat16)

                @pl.when(f != half_f)
                def _():
                    back_copy(f, e, j).start()

            loop(2, columns, far_line)

        loop(0, chunks, down)

        logits = lax.dot_general(tokb[f], router[...], NT, preferred_element_type=jnp.float32)
        s0 = jax.nn.sigmoid(jnp.sum(logits * hot[f, 0], axis=1, keepdims=True))
        s1 = jax.nn.sigmoid(jnp.sum(logits * hot[f, 1], axis=1, keepdims=True))
        weights = mask[f, 0].astype(jnp.float32) * (s0 / (s0 + s1)) + mask[f, 1].astype(jnp.float32) * (s1 / (s0 + s1))
        high = weights.astype(jnp.bfloat16)
        gates[f, 0] = high
        gates[f, 1] = (weights - high.astype(jnp.float32)).astype(jnp.bfloat16)

    def combine(f, j):
        back_arrived(f, other, j)

        @pl.when(f != half_f)
        def _():
            loop(2, columns, lambda i: back_arrived(f, lax.rem(my_y * 2 + i, columns), j))

        results = jnp.concatenate([back[f, e, :, span(j)] for e in range(columns)], axis=0)
        return (jnp.dot(gates[f, 0], results, preferred_element_type=jnp.float32)
                + jnp.dot(gates[f, 1], results, preferred_element_type=jnp.float32))

    def sum_route(d, q):
        left = jnp.logical_xor(2 * my_f >= members, q == 1)
        f = jnp.where(left, members - 1 - d, d)
        active = jnp.where(left, my_f > f, my_f < f)
        outer = jnp.where(left, my_f < members - 1, my_f > 0)
        to = jnp.where(left, my_f - 1, my_f + 1)
        index = jnp.where(both(jnp.logical_not(left), to == f), members, f)
        return f, active, outer, jnp.clip(to, 0, members - 1), index

    def sum_copy(f, j, to, index):
        return copy(rs_out.at[f, :, span(j)], rs_in.at[index, :, span(j)],
                    s_send.at[f, j], s_recv.at[index, j], dev(my_e, to))

    def sum_arrived(index, j):
        at = rs_in.at[index, :, span(j)]
        copy(at, at, s_send.at[0, j], s_recv.at[index, j], dev(my_e, my_f)).wait_recv()

    def sum_step(d, j, q):
        f, active, outer, to, index = sum_route(d, q)

        @pl.when(active)
        def _():
            total[...] = combine(f, j)

            @pl.when(outer)
            def _():
                sum_arrived(f, j)
                total[...] += rs_in[f, :, span(j)].astype(jnp.float32)

            rs_out[f, :, span(j)] = total[...].astype(jnp.bfloat16)
            sum_copy(f, j, to, index).start()

    def sum_steps(d):
        def one(i):
            @pl.when(i < chunks)
            def _():
                sum_step(d, i, 0)

            @pl.when(i > 0)
            def _():
                sum_step(d, i - 1, 1)

        loop(0, chunks + 1, one)

    shift = max(members - 3, 0)
    at_end = jnp.logical_or(my_f == 0, my_f == members - 1)

    def slot(t):
        k, j = lax.div(t, chunks), lax.rem(t, chunks)
        summing = both(k > shift, k < members + shift)

        @pl.when(k < members - 1)
        def _():
            t_step(k + 1, j)

        @pl.when(t == (members - 1) * chunks)
        def _():
            loop(0, chunks, lambda i: box(my_f, i))

        @pl.when(both(summing, both(at_end, j == 0)))
        def _():
            sum_steps(k - shift)

        turn = jnp.where(both(k == members - 2, jnp.logical_not(at_end)), chunks - 1, 0)

        @pl.when(both(j == turn, both(k >= 1, k <= members)))
        def _():
            expert(group_of(lax.rem(k, members)))

        @pl.when(both(summing, both(jnp.logical_not(at_end), j == 1)))
        def _():
            sum_steps(k - shift)

    loop(0, chunks * max(members + shift, members + 1), slot)

    def finish_own(j):
        total[...] = resid[:, span(j)].astype(jnp.float32) + combine(my_f, j)

        @pl.when(my_f < members - 1)
        def _():
            sum_arrived(my_f, j)
            total[...] += rs_in[my_f, :, span(j)].astype(jnp.float32)

        @pl.when(my_f > 0)
        def _():
            sum_arrived(members, j)
            total[...] += rs_in[members, :, span(j)].astype(jnp.float32)

        out[:, span(j)] = total[...].astype(jnp.bfloat16)

    loop(0, chunks, finish_own)

    def drain(j):
        w_start(j, True)
        t_start(j, True)
        loop(1, members, lambda s: w_step(s, j, True))
        loop(1, members, lambda d: t_step(d, j, True))
        for r in range(1, lines):
            part_copy(r, j).wait_send()

        def sums(i):
            f, active, outer, to, index = sum_route(lax.div(i, 2) + 1, lax.rem(i, 2))

            @pl.when(active)
            def _():
                sum_copy(f, j, to, index).wait_send()

        loop(0, 2 * (members - 1), sums)

    loop(0, chunks, drain)
    id_start(True)
    for r in range(1, lines):
        ctx_copy(r).wait_send()

    def drain_boxes(i):
        f, e = lax.div(i, columns), lax.rem(i, columns)

        @pl.when(e != my_e)
        def _():
            copy(outb.at[f, e], inb.at[f, my_e], b_send.at[f, e], b_recv.at[f, my_e], dev(e, my_f)).wait_send()

            @pl.when(jnp.logical_or(f != half_f, lax.div(e, 2) == my_y))
            def _():
                copy(part.at[f, e], back.at[f, my_e], r_send.at[f, e], r_recv.at[f, my_e, 0], dev(e, my_f)).wait_send()

    loop(0, members * columns, drain_boxes)
    loop(2, columns, lambda i: loop(0, chunks, lambda j: give(lax.rem(my_y * 2 + i, columns), j).wait_send()))


def on_device(tokens, context, out_proj, norm_gain, router, expert_ids, w_gate_up, w_down):
    rows, width = tokens.shape
    columns = lax.axis_size("expert")
    members = lax.axis_size("fsdp")
    n = columns * members
    experts = n // 2
    lines = columns // 2
    cap = 5 * rows // (2 * experts)
    slots = -(-cap // 8) * 8
    units = w_down.shape[1]
    k_rows = out_proj.shape[0]
    col = min(512, width)
    chunks = width // col
    others = max(lines - 1, 1)
    vmem = pl.BlockSpec(memory_space=pltpu.VMEM)
    far = pl.BlockSpec(memory_space=pl.ANY)
    bf = jnp.bfloat16
    dma = pltpu.SemaphoreType.DMA
    boxes = pltpu.VMEM((members, columns, slots, width), bf)
    marks = pltpu.VMEM((members, 2, rows, columns * slots), bf)
    call = pl.pallas_call(
        functools.partial(block_kernel, columns, members, slots, col),
        out_shape=jax.ShapeDtypeStruct((rows, width), bf),
        in_specs=[vmem] * 6 + [far] * 2,
        out_specs=vmem,
        scratch_shapes=[
            pltpu.VMEM((2 * members * k_rows, width), bf),
            pltpu.VMEM((lines, rows, 2 * members * k_rows), bf),
            pltpu.VMEM((rows, width), jnp.float32),
            pltpu.VMEM((others, rows, width), bf),
            pltpu.VMEM((others, rows, width), bf),
            pltpu.VMEM((2, units, width), bf),
            pltpu.VMEM((units, width), bf),
            pltpu.VMEM((rows, width), bf),
            pltpu.VMEM((members, 2, rows), jnp.int32),
            pltpu.VMEM((members, 2, rows, experts), jnp.float32),
            marks,
            marks,
            pltpu.VMEM((members, rows, width), bf),
            boxes, boxes,
            pltpu.VMEM((columns * slots, units), bf),
            boxes, boxes,
            pltpu.VMEM((columns, slots, width), bf),
            pltpu.VMEM((rows, col), jnp.float32),
            pltpu.VMEM((members, rows, width), bf),
            pltpu.VMEM((members + 1, rows, width), bf),
            dma((2,)), dma((members, chunks, 3)), dma((2, members, chunks)),
            dma((members, 2)), dma((members,)), dma((lines,)), dma((lines,)),
            dma((others, chunks)), dma((others, chunks)),
            dma((members, chunks, 2)), dma((members, chunks)),
            dma((members, columns)), dma((members, columns)),
            dma((members, columns)), dma((members, columns, chunks)),
            dma((columns, chunks)), dma((columns, chunks)),
            dma((members, chunks)), dma((members + 1, chunks)),
        ],
        compiler_params=pltpu.CompilerParams(
            collective_id=0, has_side_effects=True, vmem_limit_bytes=VMEM_GRANT),
    )
    return call(tokens, context, out_proj, norm_gain.reshape(1, width), router.T, expert_ids.T, w_gate_up, w_down)


def solution(mesh):
    group = ("sweep", "expert", "fsdp")
    return jax.shard_map(
        on_device,
        mesh=mesh,
        in_specs=(
            P(group, None), P(group, None), P(group, None), P("sweep"), P("sweep", None),
            P(group, None), P(group, None, None, None), P(group, None, None),
        ),
        out_specs=P(group, None),
        check_vma=False,
    )
```

```python
import functools

import jax
import jax.numpy as jnp
from jax import lax
from jax.experimental import pallas as pl
from jax.experimental.pallas import tpu as pltpu
from jax.sharding import PartitionSpec as P

eps_norm = 1e-05
MESH = pl.DeviceIdType.MESH
VMEM_GRANT = 62 * 1024 * 1024
NT = (((1,), (1,)), ((), ()))
TN = (((0,), (0,)), ((), ()))


def both(a, b):
    return jnp.logical_and(a, b)


def inside(i, n):
    return both(i >= 0, i < n)


def block_kernel(
    columns, members, slots, col,
    tok_hbm, ctx_hbm, wout_hbm, gain_hbm, router_hbm, ids_hbm, gu_hbm, dn_hbm,
    out,
    tok, ctx, gain, router, gath, ctxs, acc, pout, pin, gu, dn, resid,
    idsb, hot, mask, gates, tokb, outb, inb, hid, part, back, given, total, rs_out, rs_in,
    load_sem, out_sem, w_send, w_recv, id_send, id_recv, c_send, c_recv, p_send, p_recv,
    t_send, t_recv, b_send, b_recv, r_send, r_recv, g_send, g_recv, s_send, s_recv,
):
    lines = columns // 2
    pairs = members // 2
    experts = columns * pairs
    rows, width = tok.shape
    k_rows = wout_hbm.shape[0]
    depth = 2 * members * k_rows
    chunks = width // col
    my_e = lax.axis_index("expert")
    my_f = lax.axis_index("fsdp")
    my_y, my_c = lax.div(my_e, 2), lax.rem(my_e, 2)
    my_p = lax.div(my_f, 2)
    other = my_y * 2 + 1 - my_c
    half_f = my_f + 1 - 2 * lax.rem(my_f, 2)

    def dev(e, f):
        return {"expert": e, "fsdp": f}

    def span(j):
        return pl.ds(pl.multiple_of(j * col, col), col)

    def copy(src, dst, send, recv, target):
        return pltpu.make_async_remote_copy(
            src_ref=src, dst_ref=dst, send_sem=send, recv_sem=recv,
            device_id=target, device_id_type=MESH)

    def loop(lo, hi, body):
        def one(i, _):
            body(i)
            return 0

        lax.fori_loop(lo, hi, one, 0)

    load_gu = pltpu.make_async_copy(gu_hbm.at[0], gu, load_sem.at[0])
    load_dn = pltpu.make_async_copy(dn_hbm.at[0], dn, load_sem.at[1])

    line_part = pl.ds(pl.multiple_of(my_y * depth, depth), depth)
    mine_at = pl.ds(pl.multiple_of((my_c * members + my_f) * k_rows, k_rows), k_rows)
    loads = [
        pltpu.make_async_copy(src, dst, load_sem.at[2 + i]) for i, (src, dst) in enumerate((
            (wout_hbm, gath.at[mine_at]), (ids_hbm, idsb.at[my_f]), (ctx_hbm, ctx),
            (ctx_hbm.at[:, line_part], ctxs.at[0]), (tok_hbm, tok), (gain_hbm, gain), (router_hbm, router)))]
    for load in loads:
        load.start()

    barrier = pltpu.get_barrier_semaphore()

    def greet(e, f):
        pl.semaphore_signal(barrier, inc=1, device_id=dev(e, f), device_id_type=MESH)

    for sign in (1, -1):
        @pl.when(inside(my_f + sign, members))
        def _():
            greet(my_e, my_f + sign)

    loop(1, columns, lambda i: greet(lax.rem(my_e + i, columns), my_f))
    beside = jnp.where(my_f > 0, 1, 0) + jnp.where(my_f < members - 1, 1, 0)
    pl.semaphore_wait(barrier, columns - 1 + beside)

    for load in loads[:3]:
        load.wait()

    def place(c, f):
        return pl.ds(pl.multiple_of((c * members + f) * k_rows, k_rows), k_rows)

    def w_copy(f, j, way, target):
        at = gath.at[place(my_c, f), span(j)]
        return copy(at, at,
                    w_send.at[f, j, way], w_recv.at[my_c, f, j], target)

    def w_arrived(c, f, j):
        at = gath.at[place(c, f), span(j)]
        copy(at, at, w_send.at[f, j, 0], w_recv.at[c, f, j], dev(other, my_f)).wait_recv()

    def id_copy(f, way, target):
        return copy(idsb.at[f], idsb.at[f], id_send.at[f, way], id_recv.at[f], target)

    def ctx_copy(r):
        line = lax.rem(my_y + r, lines)
        at = pl.ds(pl.multiple_of(line * depth, depth), depth)
        return copy(ctx.at[:, at], ctxs.at[lines - r], c_send.at[r], c_recv.at[lines - r],
                    dev(line * 2 + my_c, my_f))

    def w_start(j, finish):
        for way, sign in ((0, 1), (1, -1)):
            to = my_f + sign

            @pl.when(inside(to, members))
            def _():
                mine = w_copy(my_f, j, way, dev(my_e, to))
                mine.wait_send() if finish else mine.start()
        mine = w_copy(my_f, j, 2, dev(other, my_f))
        mine.wait_send() if finish else mine.start()

    def id_start(finish):
        for way, sign in ((0, 1), (1, -1)):
            to = my_f + sign

            @pl.when(inside(to, members))
            def _():
                mine = id_copy(my_f, way, dev(my_e, to))
                mine.wait_send() if finish else mine.start()

    def w_step(s, j, finish=False):
        for way, sign in ((0, 1), (1, -1)):
            fb, to = my_f - sign * s, my_f + sign

            @pl.when(inside(fb, members))
            def _():
                if not finish:
                    w_arrived(my_c, fb, j)

                    @pl.when(j == 0)
                    def _():
                        id_copy(fb, way, dev(my_e, my_f)).wait_recv()

                @pl.when(inside(to, members))
                def _():
                    onward = w_copy(fb, j, way, dev(my_e, to))
                    onward.wait_send() if finish else onward.start()

                    @pl.when(j == 0)
                    def _():
                        named = id_copy(fb, way, dev(my_e, to))
                        named.wait_send() if finish else named.start()

                across = w_copy(fb, j, 2, dev(other, my_f))
                across.wait_send() if finish else across.start()

    loop(0, chunks, lambda j: w_start(j, False))
    id_start(False)
    for r in range(1, lines):
        ctx_copy(r).start()
    load_gu.start()
    load_dn.start()
    for load in loads[3:]:
        load.wait()

    inner = jnp.where(2 * my_f >= members, -1, 1)


    def group_of(k):
        m = jnp.minimum(my_f, members - 1 - my_f)
        half = lax.div(k + 1, 2)
        near = jnp.where(lax.rem(k, 2) == 1, my_f + inner * half, my_f - inner * half)
        return jnp.where(k <= 2 * m, near, my_f + inner * (k - m))

    def make_masks(f):
        diagonal = jnp.where(
            lax.broadcasted_iota(jnp.int32, (rows, rows), 0) == lax.broadcasted_iota(jnp.int32, (rows, rows), 1),
            1.0, 0.0)
        names = idsb[f].astype(jnp.float32)
        id0 = jnp.sum(diagonal * names[0:1], axis=1, keepdims=True).astype(jnp.int32)
        id1 = jnp.sum(diagonal * names[1:2], axis=1, keepdims=True).astype(jnp.int32)
        every = lax.broadcasted_iota(jnp.int32, (rows, experts), 1)
        hot[f, 0] = jnp.where(every == id0, 1.0, 0.0)
        hot[f, 1] = jnp.where(every == id1, 1.0, 0.0)
        place_no = lax.broadcasted_iota(jnp.int32, (rows, columns), 1)
        here = place_no * pairs + my_p
        hot0 = jnp.where(here == id0, 1.0, 0.0)
        hot1 = jnp.where(here == id1, 1.0, 0.0)
        earlier = jnp.where(
            lax.broadcasted_iota(jnp.int32, (rows, rows), 1) < lax.broadcasted_iota(jnp.int32, (rows, rows), 0),
            1.0, 0.0).astype(jnp.bfloat16)
        before = jnp.dot(earlier, (hot0 + hot1).astype(jnp.bfloat16), preferred_element_type=jnp.float32)
        spot = before + (place_no * slots + 1).astype(jnp.float32)
        slot0 = jnp.sum(spot * hot0, axis=1, keepdims=True).astype(jnp.int32) - 1
        slot1 = jnp.sum(spot * hot1, axis=1, keepdims=True).astype(jnp.int32) - 1
        slot_no = lax.broadcasted_iota(jnp.int32, (rows, columns * slots), 1)
        mask[f, 0] = jnp.where(slot_no == slot0, 1.0, 0.0).astype(jnp.bfloat16)
        mask[f, 1] = jnp.where(slot_no == slot1, 1.0, 0.0).astype(jnp.bfloat16)

    def part_copy(r, j):
        line = lax.rem(my_y + r, lines)
        return copy(pout.at[r - 1, :, span(j)], pin.at[lines - r - 1, :, span(j)],
                    p_send.at[r - 1, j], p_recv.at[lines - r - 1, j], dev(line * 2 + my_c, my_f))

    def project(j):
        loop(0, members, lambda f: w_arrived(1 - my_c, f, j))
        mixed = jnp.dot(ctxs[...].reshape(lines * rows, depth), gath[:, span(j)],
                        preferred_element_type=jnp.float32)
        for r in range(1, lines):
            pout[r - 1, :, span(j)] = mixed[r * rows:(r + 1) * rows].astype(jnp.bfloat16)
            part_copy(r, j).start()
        acc[:, span(j)] = mixed[:rows] + tok[:, span(j)].astype(jnp.float32)

    farthest = jnp.maximum(my_f, members - 1 - my_f)

    def gather(i):
        s, j = 1 + lax.div(i, chunks), lax.rem(i, chunks)

        @pl.when(s == farthest)
        def _():
            @pl.when(j == 0)
            def _():
                for r in range(1, lines):
                    ctx_copy(r).wait_recv()

            loop(lax.div(j * members, chunks), lax.div((j + 1) * members, chunks),
                 lambda k: make_masks(group_of(k)))

        w_step(s, j)

        @pl.when(s == farthest)
        def _():
            project(j)

    loop(0, (members - 1) * chunks, gather)

    if lines > 1:
        def add_parts(j):
            for r in range(1, lines):
                part_copy(r, j).wait_recv()
                acc[:, span(j)] += pin[lines - r - 1, :, span(j)].astype(jnp.float32)

        loop(0, chunks, add_parts)

    rounded = acc[...].astype(jnp.bfloat16)
    resid[...] = rounded
    widened = rounded.astype(jnp.float32)
    inv = lax.rsqrt(jnp.mean(widened * widened, axis=1, keepdims=True) + eps_norm)
    tokb[my_f] = (widened * inv * gain[...]).astype(jnp.bfloat16)

    def t_copy(f, j, way, target):
        at = tokb.at[f, :, span(j)]
        return copy(at, at, t_send.at[f, j, way], t_recv.at[f, j], target)

    def t_start(j, finish):
        for way, sign in ((0, 1), (1, -1)):
            to = my_f + sign

            @pl.when(inside(to, members))
            def _():
                mine = t_copy(my_f, j, way, dev(my_e, to))
                mine.wait_send() if finish else mine.start()

    def box_copy(f, e, j):
        return copy(outb.at[f, e, :, span(j)], inb.at[f, my_e, :, span(j)],
                    b_send.at[f, e], b_recv.at[f, my_e], dev(e, my_f))

    def box(f, j):
        boxed = lax.dot_general(mask[f, 0] + mask[f, 1], tokb[f, :, span(j)], TN,
                                preferred_element_type=jnp.float32).astype(jnp.bfloat16)
        for e in range(columns):
            outb[f, e, :, span(j)] = boxed[e * slots:(e + 1) * slots]
        loop(1, columns, lambda i: box_copy(f, lax.rem(my_e + i, columns), j).start())
        inb[f, my_e, :, span(j)] = outb[f, my_e, :, span(j)]

    def t_step(k, j, finish=False):
        f = group_of(k)
        step = jnp.where(f < my_f, 1, -1)
        to = my_f + step
        onward = t_copy(f, j, 0, dev(my_e, jnp.clip(to, 0, members - 1)))
        if not finish:
            onward.wait_recv()

        @pl.when(inside(to, members))
        def _():
            onward.wait_send() if finish else onward.start()

        if not finish:
            box(f, j)

    loop(0, chunks, lambda j: t_start(j, False))
    nothing = jnp.zeros((slots, width), jnp.bfloat16)
    loop(2, columns, lambda i: back.__setitem__((half_f, lax.rem(my_y * 2 + i, columns)), nothing))
    load_gu.wait()
    load_dn.wait()

    def back_copy(f, e, j):
        return copy(part.at[f, e, :, span(j)], back.at[f, my_e, :, span(j)],
                    r_send.at[f, e], r_recv.at[f, my_e, j], dev(e, my_f))

    def back_arrived(f, e, j):
        copy(part.at[f, e, :, span(j)], back.at[f, e, :, span(j)],
             r_send.at[f, e], r_recv.at[f, e, j], dev(e, my_f)).wait_recv()


    def give(e, j):
        return copy(part.at[half_f, e, :, span(j)], given.at[e, :, span(j)],
                    g_send.at[e, j], g_recv.at[e, j], dev(my_e, half_f))

    def expert(f):
        def boxes_arrived(i):
            e = lax.rem(my_e + i, columns)
            copy(outb.at[f, e], inb.at[f, e], b_send.at[f, e], b_recv.at[f, e], dev(e, my_f)).wait_recv()

        loop(1, columns, boxes_arrived)
        x = jnp.concatenate([inb[f, e] for e in range(columns)], axis=0)
        gate = lax.dot_general(x, gu[0], NT, preferred_element_type=jnp.float32)
        up = lax.dot_general(x, gu[1], NT, preferred_element_type=jnp.float32)
        hid[...] = (gate / (1.0 + jnp.exp(-gate)) * up).astype(jnp.bfloat16)

        def down(j):
            piece = jnp.dot(hid[...], dn[:, span(j)], preferred_element_type=jnp.float32).astype(jnp.bfloat16)
            for e in range(columns):
                part[f, e, :, span(j)] = piece[e * slots:(e + 1) * slots]
            back_copy(f, other, j).start()
            back[f, my_e, :, span(j)] = part[f, my_e, :, span(j)]

            def far_line(i):
                e = lax.rem(my_y * 2 + i, columns)

                @pl.when(f == half_f)
                def _():
                    give(e, j).start()

                @pl.when(f == my_f)
                def _():
                    give(e, j).wait_recv()
                    part[f, e, :, span(j)] = (part[f, e, :, span(j)].astype(jnp.float32)
                                              + given[e, :, span(j)].astype(jnp.float32)).astype(jnp.bfloat16)

                @pl.when(f != half_f)
                def _():
                    back_copy(f, e, j).start()

            loop(2, columns, far_line)

        loop(0, chunks, down)

        logits = lax.dot_general(tokb[f], router[...], NT, preferred_element_type=jnp.float32)
        s0 = jax.nn.sigmoid(jnp.sum(logits * hot[f, 0], axis=1, keepdims=True))
        s1 = jax.nn.sigmoid(jnp.sum(logits * hot[f, 1], axis=1, keepdims=True))
        weights = mask[f, 0].astype(jnp.float32) * (s0 / (s0 + s1)) + mask[f, 1].astype(jnp.float32) * (s1 / (s0 + s1))
        high = weights.astype(jnp.bfloat16)
        gates[f, 0] = high
        gates[f, 1] = (weights - high.astype(jnp.float32)).astype(jnp.bfloat16)

    def combine(f, j):
        back_arrived(f, other, j)

        @pl.when(f != half_f)
        def _():
            loop(2, columns, lambda i: back_arrived(f, lax.rem(my_y * 2 + i, columns), j))

        results = jnp.concatenate([back[f, e, :, span(j)] for e in range(columns)], axis=0)
        return (jnp.dot(gates[f, 0], results, preferred_element_type=jnp.float32)
                + jnp.dot(gates[f, 1], results, preferred_element_type=jnp.float32))

    def sum_route(d, q):
        left = jnp.logical_xor(2 * my_f >= members, q == 1)
        f = jnp.where(left, members - 1 - d, d)
        active = jnp.where(left, my_f > f, my_f < f)
        outer = jnp.where(left, my_f < members - 1, my_f > 0)
        to = jnp.where(left, my_f - 1, my_f + 1)
        index = jnp.where(both(jnp.logical_not(left), to == f), members, f)
        return f, active, outer, jnp.clip(to, 0, members - 1), index

    def sum_copy(f, j, to, index):
        return copy(rs_out.at[f, :, span(j)], rs_in.at[index, :, span(j)],
                    s_send.at[f, j], s_recv.at[index, j], dev(my_e, to))

    def sum_arrived(index, j):
        at = rs_in.at[index, :, span(j)]
        copy(at, at, s_send.at[0, j], s_recv.at[index, j], dev(my_e, my_f)).wait_recv()

    def sum_step(d, j, q):
        f, active, outer, to, index = sum_route(d, q)

        @pl.when(active)
        def _():
            total[...] = combine(f, j)

            @pl.when(outer)
            def _():
                sum_arrived(f, j)
                total[...] += rs_in[f, :, span(j)].astype(jnp.float32)

            rs_out[f, :, span(j)] = total[...].astype(jnp.bfloat16)
            sum_copy(f, j, to, index).start()

    def sum_steps(d):
        def one(i):
            @pl.when(i < chunks)
            def _():
                sum_step(d, i, 0)

            @pl.when(i > 0)
            def _():
                sum_step(d, i - 1, 1)

        loop(0, chunks + 1, one)

    shift = max(members - 3, 0)
    at_end = jnp.logical_or(my_f == 0, my_f == members - 1)

    def slot(t):
        k, j = lax.div(t, chunks), lax.rem(t, chunks)
        summing = both(k > shift, k < members + shift)

        @pl.when(k < members - 1)
        def _():
            t_step(k + 1, j)

        @pl.when(t == (members - 1) * chunks)
        def _():
            loop(0, chunks, lambda i: box(my_f, i))

        early = both(k == 1, j == 1)
        usual = both(j == 0, both(k > shift + 1, k < members + shift))

        @pl.when(both(at_end, jnp.logical_or(early, usual)))
        def _():
            sum_steps(jnp.where(early, 1, k - shift))

        turn = jnp.where(both(k == members - 2, jnp.logical_not(at_end)), chunks - 1, 0)

        @pl.when(both(j == turn, both(k >= 1, k <= members)))
        def _():
            expert(group_of(lax.rem(k, members)))

        @pl.when(both(summing, both(jnp.logical_not(at_end), j == 1)))
        def _():
            sum_steps(k - shift)

    loop(0, chunks * max(members + shift, members + 1), slot)

    def out_copy(j):
        return pltpu.make_async_copy(tok.at[:, span(j)], out.at[:, span(j)], out_sem.at[j])

    def finish_own(j):
        total[...] = resid[:, span(j)].astype(jnp.float32) + combine(my_f, j)

        @pl.when(my_f < members - 1)
        def _():
            sum_arrived(my_f, j)
            total[...] += rs_in[my_f, :, span(j)].astype(jnp.float32)

        @pl.when(my_f > 0)
        def _():
            sum_arrived(members, j)
            total[...] += rs_in[members, :, span(j)].astype(jnp.float32)

        out[:, span(j)] = total[...].astype(jnp.bfloat16)

    def drain(j):
        w_start(j, True)
        t_start(j, True)
        loop(1, members, lambda s: w_step(s, j, True))
        loop(1, members, lambda d: t_step(d, j, True))
        for r in range(1, lines):
            part_copy(r, j).wait_send()

    loop(0, chunks, drain)
    id_start(True)
    for r in range(1, lines):
        ctx_copy(r).wait_send()

    def drain_boxes(i):
        f, e = lax.div(i, columns), lax.rem(i, columns)

        @pl.when(e != my_e)
        def _():
            copy(outb.at[f, e], inb.at[f, my_e], b_send.at[f, e], b_recv.at[f, my_e], dev(e, my_f)).wait_send()

            @pl.when(jnp.logical_or(f != half_f, lax.div(e, 2) == my_y))
            def _():
                copy(part.at[f, e], back.at[f, my_e], r_send.at[f, e], r_recv.at[f, my_e, 0], dev(e, my_f)).wait_send()

    loop(0, members * columns, drain_boxes)
    loop(2, columns, lambda i: loop(0, chunks, lambda j: give(lax.rem(my_y * 2 + i, columns), j).wait_send()))

    loop(0, chunks, finish_own)

    def sums(i):
        f, active, outer, to, index = sum_route(lax.div(i, 2) + 1, lax.rem(i, 2))

        @pl.when(active)
        def _():
            loop(0, chunks, lambda j: sum_copy(f, j, to, index).wait_send())

    loop(0, 2 * (members - 1), sums)


def on_device(tokens, context, out_proj, norm_gain, router, expert_ids, w_gate_up, w_down):
    rows, width = tokens.shape
    columns = lax.axis_size("expert")
    members = lax.axis_size("fsdp")
    n = columns * members
    experts = n // 2
    lines = columns // 2
    cap = 5 * rows // (2 * experts)
    slots = -(-cap // 8) * 8
    units = w_down.shape[1]
    k_rows = out_proj.shape[0]
    col = min(512, width)
    chunks = width // col
    others = max(lines - 1, 1)
    far = pl.BlockSpec(memory_space=pl.ANY)
    bf = jnp.bfloat16
    dma = pltpu.SemaphoreType.DMA
    boxes = pltpu.VMEM((members, columns, slots, width), bf)
    marks = pltpu.VMEM((members, 2, rows, columns * slots), bf)
    call = pl.pallas_call(
        functools.partial(block_kernel, columns, members, slots, col),
        out_shape=pltpu.VMEM((rows, width), bf),
        in_specs=[far] * 8,
        out_specs=pl.BlockSpec(memory_space=pltpu.VMEM),
        scratch_shapes=[
            pltpu.VMEM((rows, width), bf),
            pltpu.VMEM((rows, columns // 2 * 2 * members * k_rows), bf),
            pltpu.VMEM((1, width), jnp.float32),
            pltpu.VMEM((experts, width), bf),
            pltpu.VMEM((2 * members * k_rows, width), bf),
            pltpu.VMEM((lines, rows, 2 * members * k_rows), bf),
            pltpu.VMEM((rows, width), jnp.float32),
            pltpu.VMEM((others, rows, width), bf),
            pltpu.VMEM((others, rows, width), bf),
            pltpu.VMEM((2, units, width), bf),
            pltpu.VMEM((units, width), bf),
            pltpu.VMEM((rows, width), bf),
            pltpu.VMEM((members, 2, rows), jnp.int32),
            pltpu.VMEM((members, 2, rows, experts), jnp.float32),
            marks,
            marks,
            pltpu.VMEM((members, rows, width), bf),
            boxes, boxes,
            pltpu.VMEM((columns * slots, units), bf),
            boxes, boxes,
            pltpu.VMEM((columns, slots, width), bf),
            pltpu.VMEM((rows, col), jnp.float32),
            pltpu.VMEM((members, rows, width), bf),
            pltpu.VMEM((members + 1, rows, width), bf),
            dma((9,)), dma((chunks,)), dma((members, chunks, 3)), dma((2, members, chunks)),
            dma((members, 2)), dma((members,)), dma((lines,)), dma((lines,)),
            dma((others, chunks)), dma((others, chunks)),
            dma((members, chunks, 2)), dma((members, chunks)),
            dma((members, columns)), dma((members, columns)),
            dma((members, columns)), dma((members, columns, chunks)),
            dma((columns, chunks)), dma((columns, chunks)),
            dma((members, chunks)), dma((members + 1, chunks)),
        ],
        compiler_params=pltpu.CompilerParams(
            collective_id=0, has_side_effects=True, vmem_limit_bytes=VMEM_GRANT),
    )
    return call(tokens, context, out_proj, norm_gain.reshape(1, width), router.T, expert_ids.T, w_gate_up, w_down)


def solution(mesh):
    group = ("sweep", "expert", "fsdp")
    return jax.shard_map(
        on_device,
        mesh=mesh,
        in_specs=(
            P(group, None), P(group, None), P(group, None), P("sweep"), P("sweep", None),
            P(group, None), P(group, None, None, None), P(group, None, None),
        ),
        out_specs=P(group, None),
        check_vma=False,
    )
```

```python
import functools

import jax
import jax.numpy as jnp
from jax import lax
from jax.experimental import pallas as pl
from jax.experimental.pallas import tpu as pltpu
from jax.sharding import PartitionSpec as P

eps_norm = 1e-05
MESH = pl.DeviceIdType.MESH
VMEM_GRANT = 62 * 1024 * 1024
NT = (((1,), (1,)), ((), ()))
TN = (((0,), (0,)), ((), ()))


def both(a, b):
    return jnp.logical_and(a, b)


def inside(i, n):
    return both(i >= 0, i < n)


def block_kernel(
    columns, members, slots, col,
    tok_hbm, ctx_hbm, wout_hbm, gain_hbm, router_hbm, ids_hbm, gu_hbm, dn_hbm,
    out,
    tok, ctx, gain, router, gath, ctxs, acc, pout, pin, gu, dn, resid,
    idsb, hot, mask, gates, tokb, outb, inb, hid, part, back, given, total, rs_out, rs_in,
    load_sem, out_sem, w_send, w_recv, id_send, id_recv, c_send, c_recv, p_send, p_recv,
    t_send, t_recv, b_send, b_recv, r_send, r_recv, g_send, g_recv, s_send, s_recv,
):
    lines = columns // 2
    pairs = members // 2
    experts = columns * pairs
    rows, width = tok.shape
    k_rows = wout_hbm.shape[0]
    depth = 2 * members * k_rows
    chunks = width // col
    my_e = lax.axis_index("expert")
    my_f = lax.axis_index("fsdp")
    my_y, my_c = lax.div(my_e, 2), lax.rem(my_e, 2)
    my_p = lax.div(my_f, 2)
    other = my_y * 2 + 1 - my_c
    half_f = my_f + 1 - 2 * lax.rem(my_f, 2)

    def dev(e, f):
        return {"expert": e, "fsdp": f}

    def span(j):
        return pl.ds(pl.multiple_of(j * col, col), col)

    def copy(src, dst, send, recv, target):
        return pltpu.make_async_remote_copy(
            src_ref=src, dst_ref=dst, send_sem=send, recv_sem=recv,
            device_id=target, device_id_type=MESH)

    def loop(lo, hi, body):
        def one(i, _):
            body(i)
            return 0

        lax.fori_loop(lo, hi, one, 0)

    load_gu = pltpu.make_async_copy(gu_hbm.at[0], gu, load_sem.at[0])
    load_dn = pltpu.make_async_copy(dn_hbm.at[0], dn, load_sem.at[1])

    line_part = pl.ds(pl.multiple_of(my_y * depth, depth), depth)
    mine_at = pl.ds(pl.multiple_of((my_c * members + my_f) * k_rows, k_rows), k_rows)
    loads = [
        pltpu.make_async_copy(src, dst, load_sem.at[2 + i]) for i, (src, dst) in enumerate((
            (wout_hbm, gath.at[mine_at]), (ids_hbm, idsb.at[my_f]), (ctx_hbm, ctx),
            (ctx_hbm.at[:, line_part], ctxs.at[0]), (tok_hbm, tok), (gain_hbm, gain), (router_hbm, router)))]
    for load in loads:
        load.start()

    barrier = pltpu.get_barrier_semaphore()

    def greet(e, f):
        pl.semaphore_signal(barrier, inc=1, device_id=dev(e, f), device_id_type=MESH)

    for sign in (1, -1):
        @pl.when(inside(my_f + sign, members))
        def _():
            greet(my_e, my_f + sign)

    loop(1, columns, lambda i: greet(lax.rem(my_e + i, columns), my_f))
    beside = jnp.where(my_f > 0, 1, 0) + jnp.where(my_f < members - 1, 1, 0)
    pl.semaphore_wait(barrier, columns - 1 + beside)

    for load in loads[:3]:
        load.wait()

    def place(c, f):
        return pl.ds(pl.multiple_of((c * members + f) * k_rows, k_rows), k_rows)

    def w_copy(f, j, way, target):
        at = gath.at[place(my_c, f), span(j)]
        return copy(at, at,
                    w_send.at[f, j, way], w_recv.at[my_c, f, j], target)

    def w_arrived(c, f, j):
        at = gath.at[place(c, f), span(j)]
        copy(at, at, w_send.at[f, j, 0], w_recv.at[c, f, j], dev(other, my_f)).wait_recv()

    def id_copy(f, way, target):
        return copy(idsb.at[f], idsb.at[f], id_send.at[f, way], id_recv.at[f], target)

    def ctx_copy(r):
        line = lax.rem(my_y + r, lines)
        at = pl.ds(pl.multiple_of(line * depth, depth), depth)
        return copy(ctx.at[:, at], ctxs.at[lines - r], c_send.at[r], c_recv.at[lines - r],
                    dev(line * 2 + my_c, my_f))

    def w_start(j, finish):
        for way, sign in ((0, 1), (1, -1)):
            to = my_f + sign

            @pl.when(inside(to, members))
            def _():
                mine = w_copy(my_f, j, way, dev(my_e, to))
                mine.wait_send() if finish else mine.start()
        mine = w_copy(my_f, j, 2, dev(other, my_f))
        mine.wait_send() if finish else mine.start()

    def id_start(finish):
        for way, sign in ((0, 1), (1, -1)):
            to = my_f + sign

            @pl.when(inside(to, members))
            def _():
                mine = id_copy(my_f, way, dev(my_e, to))
                mine.wait_send() if finish else mine.start()

    def w_step(s, j, finish=False):
        for way, sign in ((0, 1), (1, -1)):
            fb, to = my_f - sign * s, my_f + sign

            @pl.when(inside(fb, members))
            def _():
                if not finish:
                    w_arrived(my_c, fb, j)

                    @pl.when(j == 0)
                    def _():
                        id_copy(fb, way, dev(my_e, my_f)).wait_recv()

                @pl.when(inside(to, members))
                def _():
                    onward = w_copy(fb, j, way, dev(my_e, to))
                    onward.wait_send() if finish else onward.start()

                    @pl.when(j == 0)
                    def _():
                        named = id_copy(fb, way, dev(my_e, to))
                        named.wait_send() if finish else named.start()

                across = w_copy(fb, j, 2, dev(other, my_f))
                across.wait_send() if finish else across.start()

    loop(0, chunks, lambda j: w_start(j, False))
    id_start(False)
    for r in range(1, lines):
        ctx_copy(r).start()
    load_gu.start()
    load_dn.start()
    for load in loads[3:]:
        load.wait()

    inner = jnp.where(2 * my_f >= members, -1, 1)


    def group_of(k):
        m = jnp.minimum(my_f, members - 1 - my_f)
        half = lax.div(k + 1, 2)
        near = jnp.where(lax.rem(k, 2) == 1, my_f + inner * half, my_f - inner * half)
        return jnp.where(k <= 2 * m, near, my_f + inner * (k - m))

    def make_masks(f):
        diagonal = jnp.where(
            lax.broadcasted_iota(jnp.int32, (rows, rows), 0) == lax.broadcasted_iota(jnp.int32, (rows, rows), 1),
            1.0, 0.0)
        names = idsb[f].astype(jnp.float32)
        id0 = jnp.sum(diagonal * names[0:1], axis=1, keepdims=True).astype(jnp.int32)
        id1 = jnp.sum(diagonal * names[1:2], axis=1, keepdims=True).astype(jnp.int32)
        every = lax.broadcasted_iota(jnp.int32, (rows, experts), 1)
        hot[f, 0] = jnp.where(every == id0, 1.0, 0.0)
        hot[f, 1] = jnp.where(every == id1, 1.0, 0.0)
        place_no = lax.broadcasted_iota(jnp.int32, (rows, columns), 1)
        here = place_no * pairs + my_p
        hot0 = jnp.where(here == id0, 1.0, 0.0)
        hot1 = jnp.where(here == id1, 1.0, 0.0)
        earlier = jnp.where(
            lax.broadcasted_iota(jnp.int32, (rows, rows), 1) < lax.broadcasted_iota(jnp.int32, (rows, rows), 0),
            1.0, 0.0).astype(jnp.bfloat16)
        before = jnp.dot(earlier, (hot0 + hot1).astype(jnp.bfloat16), preferred_element_type=jnp.float32)
        spot = before + (place_no * slots + 1).astype(jnp.float32)
        slot0 = jnp.sum(spot * hot0, axis=1, keepdims=True).astype(jnp.int32) - 1
        slot1 = jnp.sum(spot * hot1, axis=1, keepdims=True).astype(jnp.int32) - 1
        slot_no = lax.broadcasted_iota(jnp.int32, (rows, columns * slots), 1)
        mask[f, 0] = jnp.where(slot_no == slot0, 1.0, 0.0).astype(jnp.bfloat16)
        mask[f, 1] = jnp.where(slot_no == slot1, 1.0, 0.0).astype(jnp.bfloat16)

    def part_copy(r, j):
        line = lax.rem(my_y + r, lines)
        return copy(pout.at[r - 1, :, span(j)], pin.at[lines - r - 1, :, span(j)],
                    p_send.at[r - 1, j], p_recv.at[lines - r - 1, j], dev(line * 2 + my_c, my_f))

    def project(j):
        loop(0, members, lambda f: w_arrived(1 - my_c, f, j))
        mixed = jnp.dot(ctxs[...].reshape(lines * rows, depth), gath[:, span(j)],
                        preferred_element_type=jnp.float32)
        for r in range(1, lines):
            pout[r - 1, :, span(j)] = mixed[r * rows:(r + 1) * rows].astype(jnp.bfloat16)
            part_copy(r, j).start()
        acc[:, span(j)] = mixed[:rows] + tok[:, span(j)].astype(jnp.float32)

    farthest = jnp.maximum(my_f, members - 1 - my_f)

    def gather(i):
        s, j = 1 + lax.div(i, chunks), lax.rem(i, chunks)

        @pl.when(s == farthest)
        def _():
            @pl.when(j == 0)
            def _():
                for r in range(1, lines):
                    ctx_copy(r).wait_recv()

            loop(lax.div(j * members, chunks), lax.div((j + 1) * members, chunks),
                 lambda k: make_masks(group_of(k)))

        w_step(s, j)

        @pl.when(s == farthest)
        def _():
            project(j)

    loop(0, (members - 1) * chunks, gather)

    if lines > 1:
        def add_parts(j):
            for r in range(1, lines):
                part_copy(r, j).wait_recv()
                acc[:, span(j)] += pin[lines - r - 1, :, span(j)].astype(jnp.float32)

        loop(0, chunks, add_parts)

    rounded = acc[...].astype(jnp.bfloat16)
    resid[...] = rounded
    widened = rounded.astype(jnp.float32)
    inv = lax.rsqrt(jnp.mean(widened * widened, axis=1, keepdims=True) + eps_norm)
    tokb[my_f] = (widened * inv * gain[...]).astype(jnp.bfloat16)

    def t_copy(f, j, way, target):
        at = tokb.at[f, :, span(j)]
        return copy(at, at, t_send.at[f, j, way], t_recv.at[f, j], target)

    def t_start(j, finish):
        for way, sign in ((0, 1), (1, -1)):
            to = my_f + sign

            @pl.when(inside(to, members))
            def _():
                mine = t_copy(my_f, j, way, dev(my_e, to))
                mine.wait_send() if finish else mine.start()

    def box_copy(f, e, j):
        return copy(outb.at[f, e, :, span(j)], inb.at[f, my_e, :, span(j)],
                    b_send.at[f, e], b_recv.at[f, my_e], dev(e, my_f))

    def box(f, j):
        boxed = lax.dot_general(mask[f, 0] + mask[f, 1], tokb[f, :, span(j)], TN,
                                preferred_element_type=jnp.float32).astype(jnp.bfloat16)
        for e in range(columns):
            outb[f, e, :, span(j)] = boxed[e * slots:(e + 1) * slots]
        loop(2, columns, lambda i: box_copy(f, lax.rem(my_y * 2 + i, columns), j).start())
        box_copy(f, other, j).start()
        inb[f, my_e, :, span(j)] = outb[f, my_e, :, span(j)]

    def t_step(k, j, finish=False):
        f = group_of(k)
        step = jnp.where(f < my_f, 1, -1)
        to = my_f + step
        onward = t_copy(f, j, 0, dev(my_e, jnp.clip(to, 0, members - 1)))
        if not finish:
            onward.wait_recv()

        @pl.when(inside(to, members))
        def _():
            onward.wait_send() if finish else onward.start()

        if not finish:
            box(f, j)

    loop(0, chunks, lambda j: t_start(j, False))
    load_gu.wait()
    load_dn.wait()

    def back_copy(f, e, j):
        return copy(part.at[f, e, :, span(j)], back.at[f, my_e, :, span(j)],
                    r_send.at[f, e], r_recv.at[f, my_e, j], dev(e, my_f))

    def back_arrived(f, e, j):
        copy(part.at[f, e, :, span(j)], back.at[f, e, :, span(j)],
             r_send.at[f, e], r_recv.at[f, e, j], dev(e, my_f)).wait_recv()


    def give(e, j):
        return copy(part.at[half_f, e, :, span(j)], given.at[e, :, span(j)],
                    g_send.at[e, j], g_recv.at[e, j], dev(my_e, half_f))

    def expert(f):
        def boxes_arrived(i):
            e = lax.rem(my_e + i, columns)
            copy(outb.at[f, e], inb.at[f, e], b_send.at[f, e], b_recv.at[f, e], dev(e, my_f)).wait_recv()

        loop(1, columns, boxes_arrived)
        x = jnp.concatenate([inb[f, e] for e in range(columns)], axis=0)
        gate = lax.dot_general(x, gu[0], NT, preferred_element_type=jnp.float32)
        up = lax.dot_general(x, gu[1], NT, preferred_element_type=jnp.float32)
        hid[...] = (gate / (1.0 + jnp.exp(-gate)) * up).astype(jnp.bfloat16)

        def down(j):
            piece = jnp.dot(hid[...], dn[:, span(j)], preferred_element_type=jnp.float32).astype(jnp.bfloat16)
            for e in range(columns):
                part[f, e, :, span(j)] = piece[e * slots:(e + 1) * slots]

            @pl.when(f == half_f)
            def _():
                loop(0, columns, lambda e: give(e, j).start())

            def add_half(e):
                give(e, j).wait_recv()
                part[f, e, :, span(j)] = (part[f, e, :, span(j)].astype(jnp.float32)
                                          + given[e, :, span(j)].astype(jnp.float32)).astype(jnp.bfloat16)

            @pl.when(f == my_f)
            def _():
                loop(0, columns, add_half)

            @pl.when(f != half_f)
            def _():
                loop(2, columns, lambda i: back_copy(f, lax.rem(my_y * 2 + i, columns), j).start())
                back_copy(f, other, j).start()
                back[f, my_e, :, span(j)] = part[f, my_e, :, span(j)]

        loop(0, chunks, down)

        logits = lax.dot_general(tokb[f], router[...], NT, preferred_element_type=jnp.float32)
        s0 = jax.nn.sigmoid(jnp.sum(logits * hot[f, 0], axis=1, keepdims=True))
        s1 = jax.nn.sigmoid(jnp.sum(logits * hot[f, 1], axis=1, keepdims=True))
        weights = mask[f, 0].astype(jnp.float32) * (s0 / (s0 + s1)) + mask[f, 1].astype(jnp.float32) * (s1 / (s0 + s1))
        high = weights.astype(jnp.bfloat16)
        gates[f, 0] = high
        gates[f, 1] = (weights - high.astype(jnp.float32)).astype(jnp.bfloat16)

    def combine(f, j):
        loop(1, columns, lambda i: back_arrived(f, lax.rem(my_e + i, columns), j))
        results = jnp.concatenate([back[f, e, :, span(j)] for e in range(columns)], axis=0)
        return (jnp.dot(gates[f, 0], results, preferred_element_type=jnp.float32)
                + jnp.dot(gates[f, 1], results, preferred_element_type=jnp.float32))

    def sum_route(d, q):
        left = jnp.logical_xor(2 * my_f >= members, q == 1)
        f = jnp.where(left, members - 1 - d, d)
        outer = jnp.where(left, my_f < members - 1, my_f > 0)
        active = both(jnp.where(left, my_f > f, my_f < f), jnp.logical_or(f != half_f, outer))
        to = jnp.where(left, my_f - 1, my_f + 1)
        index = jnp.where(both(jnp.logical_not(left), to == f), members, f)
        return f, active, outer, jnp.clip(to, 0, members - 1), index

    def sum_copy(f, j, to, index):
        return copy(rs_out.at[f, :, span(j)], rs_in.at[index, :, span(j)],
                    s_send.at[f, j], s_recv.at[index, j], dev(my_e, to))

    def sum_arrived(index, j):
        at = rs_in.at[index, :, span(j)]
        copy(at, at, s_send.at[0, j], s_recv.at[index, j], dev(my_e, my_f)).wait_recv()

    def sum_step(d, j, q):
        f, active, outer, to, index = sum_route(d, q)

        @pl.when(active)
        def _():
            @pl.when(f != half_f)
            def _():
                total[...] = combine(f, j)

            @pl.when(f == half_f)
            def _():
                total[...] = jnp.zeros_like(total)

            @pl.when(outer)
            def _():
                sum_arrived(f, j)
                total[...] += rs_in[f, :, span(j)].astype(jnp.float32)

            rs_out[f, :, span(j)] = total[...].astype(jnp.bfloat16)
            sum_copy(f, j, to, index).start()

    def sum_steps(d):
        def one(i):
            @pl.when(i < chunks)
            def _():
                sum_step(d, i, 0)

            @pl.when(i > 0)
            def _():
                sum_step(d, i - 1, 1)

        loop(0, chunks + 1, one)

    shift = max(members - 3, 0)
    at_end = jnp.logical_or(my_f == 0, my_f == members - 1)

    def slot(t):
        k, j = lax.div(t, chunks), lax.rem(t, chunks)
        summing = both(k > shift, k < members + shift)

        @pl.when(k < members - 1)
        def _():
            t_step(k + 1, j)

        @pl.when(both(t == (members - 1) * chunks, jnp.logical_not(at_end)))
        def _():
            loop(0, chunks, lambda i: box(my_f, i))

        usual = both(j == 0, both(k > shift + 1, k < members + shift))

        @pl.when(both(at_end, usual))
        def _():
            sum_steps(k - shift)

        turn = jnp.where(both(k == members - 2, jnp.logical_not(at_end)), chunks - 1, 0)

        @pl.when(both(j == turn, both(k >= 1, k <= members)))
        def _():
            expert(group_of(lax.rem(k, members)))

        @pl.when(both(t == (members - 1) * chunks, at_end))
        def _():
            loop(0, chunks, lambda i: box(my_f, i))

        @pl.when(both(summing, both(jnp.logical_not(at_end), j == 1)))
        def _():
            sum_steps(k - shift)

    loop(0, chunks * max(members + shift, members + 1), slot)

    def out_copy(j):
        return pltpu.make_async_copy(tok.at[:, span(j)], out.at[:, span(j)], out_sem.at[j])

    def finish_own(j):
        total[...] = resid[:, span(j)].astype(jnp.float32) + combine(my_f, j)

        @pl.when(members - 1 - my_f > 1 - lax.rem(my_f, 2))
        def _():
            sum_arrived(my_f, j)
            total[...] += rs_in[my_f, :, span(j)].astype(jnp.float32)

        @pl.when(my_f > lax.rem(my_f, 2))
        def _():
            sum_arrived(members, j)
            total[...] += rs_in[members, :, span(j)].astype(jnp.float32)

        out[:, span(j)] = total[...].astype(jnp.bfloat16)

    def drain(j):
        w_start(j, True)
        t_start(j, True)
        loop(1, members, lambda s: w_step(s, j, True))
        loop(1, members, lambda d: t_step(d, j, True))
        for r in range(1, lines):
            part_copy(r, j).wait_send()

    loop(0, chunks, drain)
    id_start(True)
    for r in range(1, lines):
        ctx_copy(r).wait_send()

    def drain_boxes(i):
        f, e = lax.div(i, columns), lax.rem(i, columns)

        @pl.when(e != my_e)
        def _():
            copy(outb.at[f, e], inb.at[f, my_e], b_send.at[f, e], b_recv.at[f, my_e], dev(e, my_f)).wait_send()

            @pl.when(f != half_f)
            def _():
                copy(part.at[f, e], back.at[f, my_e], r_send.at[f, e], r_recv.at[f, my_e, 0], dev(e, my_f)).wait_send()

    loop(0, members * columns, drain_boxes)
    loop(0, columns, lambda e: loop(0, chunks, lambda j: give(e, j).wait_send()))

    loop(0, chunks, finish_own)

    def sums(i):
        f, active, outer, to, index = sum_route(lax.div(i, 2) + 1, lax.rem(i, 2))

        @pl.when(active)
        def _():
            loop(0, chunks, lambda j: sum_copy(f, j, to, index).wait_send())

    loop(0, 2 * (members - 1), sums)


def on_device(tokens, context, out_proj, norm_gain, router, expert_ids, w_gate_up, w_down):
    rows, width = tokens.shape
    columns = lax.axis_size("expert")
    members = lax.axis_size("fsdp")
    n = columns * members
    experts = n // 2
    lines = columns // 2
    cap = 5 * rows // (2 * experts)
    slots = -(-cap // 8) * 8
    units = w_down.shape[1]
    k_rows = out_proj.shape[0]
    col = min(512, width)
    chunks = width // col
    others = max(lines - 1, 1)
    far = pl.BlockSpec(memory_space=pl.ANY)
    bf = jnp.bfloat16
    dma = pltpu.SemaphoreType.DMA
    boxes = pltpu.VMEM((members, columns, slots, width), bf)
    marks = pltpu.VMEM((members, 2, rows, columns * slots), bf)
    call = pl.pallas_call(
        functools.partial(block_kernel, columns, members, slots, col),
        out_shape=pltpu.VMEM((rows, width), bf),
        in_specs=[far] * 8,
        out_specs=pl.BlockSpec(memory_space=pltpu.VMEM),
        scratch_shapes=[
            pltpu.VMEM((rows, width), bf),
            pltpu.VMEM((rows, columns // 2 * 2 * members * k_rows), bf),
            pltpu.VMEM((1, width), jnp.float32),
            pltpu.VMEM((experts, width), bf),
            pltpu.VMEM((2 * members * k_rows, width), bf),
            pltpu.VMEM((lines, rows, 2 * members * k_rows), bf),
            pltpu.VMEM((rows, width), jnp.float32),
            pltpu.VMEM((others, rows, width), bf),
            pltpu.VMEM((others, rows, width), bf),
            pltpu.VMEM((2, units, width), bf),
            pltpu.VMEM((units, width), bf),
            pltpu.VMEM((rows, width), bf),
            pltpu.VMEM((members, 2, rows), jnp.int32),
            pltpu.VMEM((members, 2, rows, experts), jnp.float32),
            marks,
            marks,
            pltpu.VMEM((members, rows, width), bf),
            boxes, boxes,
            pltpu.VMEM((columns * slots, units), bf),
            boxes, boxes,
            pltpu.VMEM((columns, slots, width), bf),
            pltpu.VMEM((rows, col), jnp.float32),
            pltpu.VMEM((members, rows, width), bf),
            pltpu.VMEM((members + 1, rows, width), bf),
            dma((9,)), dma((chunks,)), dma((members, chunks, 3)), dma((2, members, chunks)),
            dma((members, 2)), dma((members,)), dma((lines,)), dma((lines,)),
            dma((others, chunks)), dma((others, chunks)),
            dma((members, chunks, 2)), dma((members, chunks)),
            dma((members, columns)), dma((members, columns)),
            dma((members, columns)), dma((members, columns, chunks)),
            dma((columns, chunks)), dma((columns, chunks)),
            dma((members, chunks)), dma((members + 1, chunks)),
        ],
        compiler_params=pltpu.CompilerParams(
            collective_id=0, has_side_effects=True, vmem_limit_bytes=VMEM_GRANT),
    )
    return call(tokens, context, out_proj, norm_gain.reshape(1, width), router.T, expert_ids.T, w_gate_up, w_down)


def solution(mesh):
    group = ("sweep", "expert", "fsdp")
    return jax.shard_map(
        on_device,
        mesh=mesh,
        in_specs=(
            P(group, None), P(group, None), P(group, None), P("sweep"), P("sweep", None),
            P(group, None), P(group, None, None, None), P(group, None, None),
        ),
        out_specs=P(group, None),
        check_vma=False,
    )
```

```python
import functools

import jax
import jax.numpy as jnp
from jax import lax
from jax.experimental import pallas as pl
from jax.experimental.pallas import tpu as pltpu
from jax.sharding import PartitionSpec as P

eps_norm = 1e-05
MESH = pl.DeviceIdType.MESH
VMEM_GRANT = 62 * 1024 * 1024
NT = (((1,), (1,)), ((), ()))
TN = (((0,), (0,)), ((), ()))


def both(a, b):
    return jnp.logical_and(a, b)


def inside(i, n):
    return both(i >= 0, i < n)


def block_kernel(
    columns, members, slots, col,
    tok_hbm, ctx_hbm, wout_hbm, gain_hbm, router_hbm, ids_hbm, gu_hbm, dn_hbm,
    out,
    tok, ctx, gain, router, gath, ctxs, acc, pout, pin, gu, dn, resid,
    idsb, hot, mask, gates, tokb, outb, inb, hid, part, back, given, total, rs_out, rs_in,
    load_sem, out_sem, w_send, w_recv, id_send, id_recv, c_send, c_recv, p_send, p_recv,
    t_send, t_recv, b_send, b_recv, r_send, r_recv, g_send, g_recv, s_send, s_recv,
):
    lines = columns // 2
    pairs = members // 2
    experts = columns * pairs
    rows, width = tok.shape
    k_rows = wout_hbm.shape[0]
    depth = 2 * members * k_rows
    chunks = width // col
    my_e = lax.axis_index("expert")
    my_f = lax.axis_index("fsdp")
    my_y, my_c = lax.div(my_e, 2), lax.rem(my_e, 2)
    my_p = lax.div(my_f, 2)
    other = my_y * 2 + 1 - my_c
    half_f = my_f + 1 - 2 * lax.rem(my_f, 2)

    def dev(e, f):
        return {"expert": e, "fsdp": f}

    def span(j):
        return pl.ds(pl.multiple_of(j * col, col), col)

    def copy(src, dst, send, recv, target):
        return pltpu.make_async_remote_copy(
            src_ref=src, dst_ref=dst, send_sem=send, recv_sem=recv,
            device_id=target, device_id_type=MESH)

    def loop(lo, hi, body):
        def one(i, _):
            body(i)
            return 0

        lax.fori_loop(lo, hi, one, 0)

    load_gu = pltpu.make_async_copy(gu_hbm.at[0], gu, load_sem.at[0])
    load_dn = pltpu.make_async_copy(dn_hbm.at[0], dn, load_sem.at[1])

    line_part = pl.ds(pl.multiple_of(my_y * depth, depth), depth)
    mine_at = pl.ds(pl.multiple_of((my_c * members + my_f) * k_rows, k_rows), k_rows)
    loads = [
        pltpu.make_async_copy(src, dst, load_sem.at[2 + i]) for i, (src, dst) in enumerate((
            (wout_hbm, gath.at[mine_at]), (ids_hbm, idsb.at[my_f]), (ctx_hbm, ctx),
            (ctx_hbm.at[:, line_part], ctxs.at[0]), (tok_hbm, tok), (gain_hbm, gain), (router_hbm, router)))]
    for load in loads:
        load.start()

    barrier = pltpu.get_barrier_semaphore()

    def greet(e, f):
        pl.semaphore_signal(barrier, inc=1, device_id=dev(e, f), device_id_type=MESH)

    for sign in (1, -1):
        @pl.when(inside(my_f + sign, members))
        def _():
            greet(my_e, my_f + sign)

    loop(1, columns, lambda i: greet(lax.rem(my_e + i, columns), my_f))
    beside = jnp.where(my_f > 0, 1, 0) + jnp.where(my_f < members - 1, 1, 0)
    pl.semaphore_wait(barrier, columns - 1 + beside)

    for load in loads[:3]:
        load.wait()

    def place(c, f):
        return pl.ds(pl.multiple_of((c * members + f) * k_rows, k_rows), k_rows)

    def w_copy(f, j, way, target):
        at = gath.at[place(my_c, f), span(j)]
        return copy(at, at,
                    w_send.at[f, j, way], w_recv.at[my_c, f, j], target)

    def w_arrived(c, f, j):
        at = gath.at[place(c, f), span(j)]
        copy(at, at, w_send.at[f, j, 0], w_recv.at[c, f, j], dev(other, my_f)).wait_recv()

    def id_copy(f, way, target):
        return copy(idsb.at[f], idsb.at[f], id_send.at[f, way], id_recv.at[f], target)

    def ctx_copy(r):
        line = lax.rem(my_y + r, lines)
        at = pl.ds(pl.multiple_of(line * depth, depth), depth)
        return copy(ctx.at[:, at], ctxs.at[lines - r], c_send.at[r], c_recv.at[lines - r],
                    dev(line * 2 + my_c, my_f))

    def w_start(j, finish):
        for way, sign in ((0, 1), (1, -1)):
            to = my_f + sign

            @pl.when(inside(to, members))
            def _():
                mine = w_copy(my_f, j, way, dev(my_e, to))
                mine.wait_send() if finish else mine.start()
        mine = w_copy(my_f, j, 2, dev(other, my_f))
        mine.wait_send() if finish else mine.start()

    def id_start(finish):
        for way, sign in ((0, 1), (1, -1)):
            to = my_f + sign

            @pl.when(inside(to, members))
            def _():
                mine = id_copy(my_f, way, dev(my_e, to))
                mine.wait_send() if finish else mine.start()

    def w_step(s, j, finish=False):
        for way, sign in ((0, 1), (1, -1)):
            fb, to = my_f - sign * s, my_f + sign

            @pl.when(inside(fb, members))
            def _():
                if not finish:
                    w_arrived(my_c, fb, j)

                    @pl.when(j == 0)
                    def _():
                        id_copy(fb, way, dev(my_e, my_f)).wait_recv()

                @pl.when(inside(to, members))
                def _():
                    onward = w_copy(fb, j, way, dev(my_e, to))
                    onward.wait_send() if finish else onward.start()

                    @pl.when(j == 0)
                    def _():
                        named = id_copy(fb, way, dev(my_e, to))
                        named.wait_send() if finish else named.start()

                across = w_copy(fb, j, 2, dev(other, my_f))
                across.wait_send() if finish else across.start()

    loop(0, chunks, lambda j: w_start(j, False))
    id_start(False)
    for r in range(1, lines):
        ctx_copy(r).start()
    load_gu.start()
    load_dn.start()
    for load in loads[3:]:
        load.wait()

    inner = jnp.where(2 * my_f >= members, -1, 1)


    def group_of(k):
        m = jnp.minimum(my_f, members - 1 - my_f)
        half = lax.div(k + 1, 2)
        near = jnp.where(lax.rem(k, 2) == 1, my_f + inner * half, my_f - inner * half)
        return jnp.where(k <= 2 * m, near, my_f + inner * (k - m))

    def make_masks(f):
        diagonal = jnp.where(
            lax.broadcasted_iota(jnp.int32, (rows, rows), 0) == lax.broadcasted_iota(jnp.int32, (rows, rows), 1),
            1.0, 0.0)
        names = idsb[f].astype(jnp.float32)
        id0 = jnp.sum(diagonal * names[0:1], axis=1, keepdims=True).astype(jnp.int32)
        id1 = jnp.sum(diagonal * names[1:2], axis=1, keepdims=True).astype(jnp.int32)
        every = lax.broadcasted_iota(jnp.int32, (rows, experts), 1)
        hot[f, 0] = jnp.where(every == id0, 1.0, 0.0)
        hot[f, 1] = jnp.where(every == id1, 1.0, 0.0)
        place_no = lax.broadcasted_iota(jnp.int32, (rows, columns), 1)
        here = place_no * pairs + my_p
        hot0 = jnp.where(here == id0, 1.0, 0.0)
        hot1 = jnp.where(here == id1, 1.0, 0.0)
        earlier = jnp.where(
            lax.broadcasted_iota(jnp.int32, (rows, rows), 1) < lax.broadcasted_iota(jnp.int32, (rows, rows), 0),
            1.0, 0.0).astype(jnp.bfloat16)
        before = jnp.dot(earlier, (hot0 + hot1).astype(jnp.bfloat16), preferred_element_type=jnp.float32)
        spot = before + (place_no * slots + 1).astype(jnp.float32)
        slot0 = jnp.sum(spot * hot0, axis=1, keepdims=True).astype(jnp.int32) - 1
        slot1 = jnp.sum(spot * hot1, axis=1, keepdims=True).astype(jnp.int32) - 1
        slot_no = lax.broadcasted_iota(jnp.int32, (rows, columns * slots), 1)
        mask[f, 0] = jnp.where(slot_no == slot0, 1.0, 0.0).astype(jnp.bfloat16)
        mask[f, 1] = jnp.where(slot_no == slot1, 1.0, 0.0).astype(jnp.bfloat16)

    def part_copy(r, j):
        line = lax.rem(my_y + r, lines)
        return copy(pout.at[r - 1, :, span(j)], pin.at[lines - r - 1, :, span(j)],
                    p_send.at[r - 1, j], p_recv.at[lines - r - 1, j], dev(line * 2 + my_c, my_f))

    def project(j):
        loop(0, members, lambda f: w_arrived(1 - my_c, f, j))
        mixed = jnp.dot(ctxs[...].reshape(lines * rows, depth), gath[:, span(j)],
                        preferred_element_type=jnp.float32)
        for r in range(1, lines):
            pout[r - 1, :, span(j)] = mixed[r * rows:(r + 1) * rows].astype(jnp.bfloat16)
            part_copy(r, j).start()
        acc[:, span(j)] = mixed[:rows] + tok[:, span(j)].astype(jnp.float32)

    farthest = jnp.maximum(my_f, members - 1 - my_f)

    def gather(i):
        s, j = 1 + lax.div(i, chunks), lax.rem(i, chunks)

        @pl.when(s == farthest)
        def _():
            @pl.when(j == 0)
            def _():
                for r in range(1, lines):
                    ctx_copy(r).wait_recv()

            loop(lax.div(j * members, chunks), lax.div((j + 1) * members, chunks),
                 lambda k: make_masks(group_of(k)))

        w_step(s, j)

        @pl.when(s == farthest)
        def _():
            project(j)

    loop(0, (members - 1) * chunks, gather)

    if lines > 1:
        def add_parts(j):
            for r in range(1, lines):
                part_copy(r, j).wait_recv()
                acc[:, span(j)] += pin[lines - r - 1, :, span(j)].astype(jnp.float32)

        loop(0, chunks, add_parts)

    rounded = acc[...].astype(jnp.bfloat16)
    resid[...] = rounded
    widened = rounded.astype(jnp.float32)
    inv = lax.rsqrt(jnp.mean(widened * widened, axis=1, keepdims=True) + eps_norm)
    tokb[my_f] = (widened * inv * gain[...]).astype(jnp.bfloat16)

    def t_copy(f, j, way, target):
        at = tokb.at[f, :, span(j)]
        return copy(at, at, t_send.at[f, j, way], t_recv.at[f, j], target)

    def t_start(j, finish):
        for way, sign in ((0, 1), (1, -1)):
            to = my_f + sign

            @pl.when(inside(to, members))
            def _():
                mine = t_copy(my_f, j, way, dev(my_e, to))
                mine.wait_send() if finish else mine.start()

    def box_copy(f, e, j):
        return copy(outb.at[f, e, :, span(j)], inb.at[f, my_e, :, span(j)],
                    b_send.at[f, e], b_recv.at[f, my_e], dev(e, my_f))

    def box(f, j):
        boxed = lax.dot_general(mask[f, 0] + mask[f, 1], tokb[f, :, span(j)], TN,
                                preferred_element_type=jnp.float32).astype(jnp.bfloat16)
        for e in range(columns):
            outb[f, e, :, span(j)] = boxed[e * slots:(e + 1) * slots]
        loop(2, columns, lambda i: box_copy(f, lax.rem(my_y * 2 + i, columns), j).start())
        box_copy(f, other, j).start()
        inb[f, my_e, :, span(j)] = outb[f, my_e, :, span(j)]

    def t_step(k, j, finish=False):
        f = group_of(k)
        step = jnp.where(f < my_f, 1, -1)
        to = my_f + step
        onward = t_copy(f, j, 0, dev(my_e, jnp.clip(to, 0, members - 1)))
        if not finish:
            onward.wait_recv()

        @pl.when(inside(to, members))
        def _():
            onward.wait_send() if finish else onward.start()

        if not finish:
            box(f, j)

    loop(0, chunks, lambda j: t_start(j, False))
    load_gu.wait()
    load_dn.wait()

    def back_copy(f, e, j):
        return copy(part.at[f, e, :, span(j)], back.at[f, my_e, :, span(j)],
                    r_send.at[f, e], r_recv.at[f, my_e, j], dev(e, my_f))

    def back_arrived(f, e, j):
        copy(part.at[f, e, :, span(j)], back.at[f, e, :, span(j)],
             r_send.at[f, e], r_recv.at[f, e, j], dev(e, my_f)).wait_recv()


    def give(e, j):
        return copy(part.at[half_f, e, :, span(j)], given.at[e, :, span(j)],
                    g_send.at[e, j], g_recv.at[e, j], dev(my_e, half_f))

    def expert(f):
        def boxes_arrived(i):
            e = lax.rem(my_e + i, columns)
            copy(outb.at[f, e], inb.at[f, e], b_send.at[f, e], b_recv.at[f, e], dev(e, my_f)).wait_recv()

        loop(1, columns, boxes_arrived)
        x = jnp.concatenate([inb[f, e] for e in range(columns)], axis=0)
        gate = lax.dot_general(x, gu[0], NT, preferred_element_type=jnp.float32)
        up = lax.dot_general(x, gu[1], NT, preferred_element_type=jnp.float32)
        hid[...] = (gate / (1.0 + jnp.exp(-gate)) * up).astype(jnp.bfloat16)

        def down(j):
            piece = jnp.dot(hid[...], dn[:, span(j)], preferred_element_type=jnp.float32).astype(jnp.bfloat16)
            for e in range(columns):
                part[f, e, :, span(j)] = piece[e * slots:(e + 1) * slots]

            @pl.when(f == half_f)
            def _():
                loop(0, columns, lambda e: give(e, j).start())

            def add_half(e):
                give(e, j).wait_recv()
                part[f, e, :, span(j)] = (part[f, e, :, span(j)].astype(jnp.float32)
                                          + given[e, :, span(j)].astype(jnp.float32)).astype(jnp.bfloat16)

            @pl.when(f == my_f)
            def _():
                loop(0, columns, add_half)

            @pl.when(f != half_f)
            def _():
                loop(2, columns, lambda i: back_copy(f, lax.rem(my_y * 2 + i, columns), j).start())
                back_copy(f, other, j).start()
                back[f, my_e, :, span(j)] = part[f, my_e, :, span(j)]

        loop(0, chunks, down)

        logits = lax.dot_general(tokb[f], router[...], NT, preferred_element_type=jnp.float32)
        s0 = jax.nn.sigmoid(jnp.sum(logits * hot[f, 0], axis=1, keepdims=True))
        s1 = jax.nn.sigmoid(jnp.sum(logits * hot[f, 1], axis=1, keepdims=True))
        weights = mask[f, 0].astype(jnp.float32) * (s0 / (s0 + s1)) + mask[f, 1].astype(jnp.float32) * (s1 / (s0 + s1))
        high = weights.astype(jnp.bfloat16)
        gates[f, 0] = high
        gates[f, 1] = (weights - high.astype(jnp.float32)).astype(jnp.bfloat16)

    def combine(f, j):
        loop(1, columns, lambda i: back_arrived(f, lax.rem(my_e + i, columns), j))
        results = jnp.concatenate([back[f, e, :, span(j)] for e in range(columns)], axis=0)
        return (jnp.dot(gates[f, 0], results, preferred_element_type=jnp.float32)
                + jnp.dot(gates[f, 1], results, preferred_element_type=jnp.float32))

    def sum_route(d, q):
        left = jnp.logical_xor(2 * my_f >= members, q == 1)
        f = jnp.where(left, members - 1 - d, d)
        outer = jnp.where(left, my_f < members - 1, my_f > 0)
        active = both(jnp.where(left, my_f > f, my_f < f), jnp.logical_or(f != half_f, outer))
        to = jnp.where(left, my_f - 1, my_f + 1)
        index = jnp.where(both(jnp.logical_not(left), to == f), members, f)
        return f, active, outer, jnp.clip(to, 0, members - 1), index

    def sum_copy(f, j, to, index):
        return copy(rs_out.at[f, :, span(j)], rs_in.at[index, :, span(j)],
                    s_send.at[f, j], s_recv.at[index, j], dev(my_e, to))

    def sum_arrived(index, j):
        at = rs_in.at[index, :, span(j)]
        copy(at, at, s_send.at[0, j], s_recv.at[index, j], dev(my_e, my_f)).wait_recv()

    def sum_step(d, j, q):
        f, active, outer, to, index = sum_route(d, q)

        @pl.when(active)
        def _():
            @pl.when(f != half_f)
            def _():
                total[...] = combine(f, j)

            @pl.when(f == half_f)
            def _():
                total[...] = jnp.zeros_like(total)

            @pl.when(outer)
            def _():
                sum_arrived(f, j)
                total[...] += rs_in[f, :, span(j)].astype(jnp.float32)

            rs_out[f, :, span(j)] = total[...].astype(jnp.bfloat16)
            sum_copy(f, j, to, index).start()

    def sum_steps(d):
        def one(i):
            @pl.when(i < chunks)
            def _():
                sum_step(d, i, 0)

            @pl.when(i > 0)
            def _():
                sum_step(d, i - 1, 1)

        loop(0, chunks + 1, one)

    shift = max(members - 3, 0)
    at_end = jnp.logical_or(my_f == 0, my_f == members - 1)

    def slot(t):
        k, j = lax.div(t, chunks), lax.rem(t, chunks)
        summing = both(k > shift, k < members + shift)

        @pl.when(k < members - 1)
        def _():
            t_step(k + 1, j)

        @pl.when(both(t == (members - 1) * chunks, jnp.logical_not(at_end)))
        def _():
            loop(0, chunks, lambda i: box(my_f, i))

        usual = both(j == 0, both(k > shift + 1, k < members + shift))

        @pl.when(both(at_end, usual))
        def _():
            sum_steps(k - shift)

        turn = jnp.where(k == members - 2, jnp.where(at_end, min(1, chunks - 1), chunks - 1), 0)

        @pl.when(both(j == turn, both(k >= 1, k <= members)))
        def _():
            expert(group_of(lax.rem(k, members)))

        @pl.when(both(t == (members - 1) * chunks, at_end))
        def _():
            loop(0, chunks, lambda i: box(my_f, i))

        @pl.when(both(summing, both(jnp.logical_not(at_end), j == min(1, chunks - 1))))
        def _():
            sum_steps(k - shift)

    loop(0, chunks * max(members + shift, members + 1), slot)

    def out_copy(j):
        return pltpu.make_async_copy(tok.at[:, span(j)], out.at[:, span(j)], out_sem.at[j])

    def finish_own(j):
        total[...] = resid[:, span(j)].astype(jnp.float32) + combine(my_f, j)

        @pl.when(members - 1 - my_f > 1 - lax.rem(my_f, 2))
        def _():
            sum_arrived(my_f, j)
            total[...] += rs_in[my_f, :, span(j)].astype(jnp.float32)

        @pl.when(my_f > lax.rem(my_f, 2))
        def _():
            sum_arrived(members, j)
            total[...] += rs_in[members, :, span(j)].astype(jnp.float32)

        out[:, span(j)] = total[...].astype(jnp.bfloat16)

    def drain(j):
        w_start(j, True)
        t_start(j, True)
        loop(1, members, lambda s: w_step(s, j, True))
        loop(1, members, lambda d: t_step(d, j, True))
        for r in range(1, lines):
            part_copy(r, j).wait_send()

    loop(0, chunks, drain)
    id_start(True)
    for r in range(1, lines):
        ctx_copy(r).wait_send()

    def drain_boxes(i):
        f, e = lax.div(i, columns), lax.rem(i, columns)

        @pl.when(e != my_e)
        def _():
            copy(outb.at[f, e], inb.at[f, my_e], b_send.at[f, e], b_recv.at[f, my_e], dev(e, my_f)).wait_send()

            @pl.when(f != half_f)
            def _():
                copy(part.at[f, e], back.at[f, my_e], r_send.at[f, e], r_recv.at[f, my_e, 0], dev(e, my_f)).wait_send()

    loop(0, members * columns, drain_boxes)
    loop(0, columns, lambda e: loop(0, chunks, lambda j: give(e, j).wait_send()))

    loop(0, chunks, finish_own)

    def sums(i):
        f, active, outer, to, index = sum_route(lax.div(i, 2) + 1, lax.rem(i, 2))

        @pl.when(active)
        def _():
            loop(0, chunks, lambda j: sum_copy(f, j, to, index).wait_send())

    loop(0, 2 * (members - 1), sums)


def on_device(tokens, context, out_proj, norm_gain, router, expert_ids, w_gate_up, w_down):
    rows, width = tokens.shape
    columns = lax.axis_size("expert")
    members = lax.axis_size("fsdp")
    n = columns * members
    experts = n // 2
    lines = columns // 2
    cap = 5 * rows // (2 * experts)
    slots = -(-cap // 8) * 8
    units = w_down.shape[1]
    k_rows = out_proj.shape[0]
    col = min(512, width)
    chunks = width // col
    others = max(lines - 1, 1)
    far = pl.BlockSpec(memory_space=pl.ANY)
    bf = jnp.bfloat16
    dma = pltpu.SemaphoreType.DMA
    boxes = pltpu.VMEM((members, columns, slots, width), bf)
    marks = pltpu.VMEM((members, 2, rows, columns * slots), bf)
    call = pl.pallas_call(
        functools.partial(block_kernel, columns, members, slots, col),
        out_shape=pltpu.VMEM((rows, width), bf),
        in_specs=[far] * 8,
        out_specs=pl.BlockSpec(memory_space=pltpu.VMEM),
        scratch_shapes=[
            pltpu.VMEM((rows, width), bf),
            pltpu.VMEM((rows, columns // 2 * 2 * members * k_rows), bf),
            pltpu.VMEM((1, width), jnp.float32),
            pltpu.VMEM((experts, width), bf),
            pltpu.VMEM((2 * members * k_rows, width), bf),
            pltpu.VMEM((lines, rows, 2 * members * k_rows), bf),
            pltpu.VMEM((rows, width), jnp.float32),
            pltpu.VMEM((others, rows, width), bf),
            pltpu.VMEM((others, rows, width), bf),
            pltpu.VMEM((2, units, width), bf),
            pltpu.VMEM((units, width), bf),
            pltpu.VMEM((rows, width), bf),
            pltpu.VMEM((members, 2, rows), jnp.int32),
            pltpu.VMEM((members, 2, rows, experts), jnp.float32),
            marks,
            marks,
            pltpu.VMEM((members, rows, width), bf),
            boxes, boxes,
            pltpu.VMEM((columns * slots, units), bf),
            boxes, boxes,
            pltpu.VMEM((columns, slots, width), bf),
            pltpu.VMEM((rows, col), jnp.float32),
            pltpu.VMEM((members, rows, width), bf),
            pltpu.VMEM((members + 1, rows, width), bf),
            dma((9,)), dma((chunks,)), dma((members, chunks, 3)), dma((2, members, chunks)),
            dma((members, 2)), dma((members,)), dma((lines,)), dma((lines,)),
            dma((others, chunks)), dma((others, chunks)),
            dma((members, chunks, 2)), dma((members, chunks)),
            dma((members, columns)), dma((members, columns)),
            dma((members, columns)), dma((members, columns, chunks)),
            dma((columns, chunks)), dma((columns, chunks)),
            dma((members, chunks)), dma((members + 1, chunks)),
        ],
        compiler_params=pltpu.CompilerParams(
            collective_id=0, has_side_effects=True, vmem_limit_bytes=VMEM_GRANT),
    )
    return call(tokens, context, out_proj, norm_gain.reshape(1, width), router.T, expert_ids.T, w_gate_up, w_down)


def solution(mesh):
    group = ("sweep", "expert", "fsdp")
    return jax.shard_map(
        on_device,
        mesh=mesh,
        in_specs=(
            P(group, None), P(group, None), P(group, None), P("sweep"), P("sweep", None),
            P(group, None), P(group, None, None, None), P(group, None, None),
        ),
        out_specs=P(group, None),
        check_vma=False,
    )
```
